256 devices in a mesh: grp: 16 (over x, z_lo, core), dev: 16 (over z_hi, y).
Axes of the slice: x: 4, y: 4, z: 8 (z_hi: 4, z_lo: 2; z = z_hi * 2 + z_lo), core: 2. Of those that a mesh axis runs over, the one named last changes fastest.
Arguments:
- a_tiles: float32 [8192, 3, 128, 128], P(('grp', 'dev')), may hold values from -1.7071068 to 18.707107
- prolong: float32 [8192, 2, 128, 128], P(('grp', 'dev')), may hold values from -0.5 to 0.5
- coarse_ids: int32 [8192, 2], P(('grp', 'dev')), may hold values from 0 to 3, as said below
Outputs:
- coarse: float32 [8192, 1536], P(('grp', 'dev'))
The draws below stay inside these ranges and needn't reach their ends.
Inputs may be any that keep to these rules, and one draw needn't show every extreme that they name: `coarse_ids`: each fine block names 2 different coarse tiles, numbered within its own group.
All inputs are finite; a program needn't handle non-finite values.
Results may differ from the reference program's by a relative error of at most 0.0001.
Values sent between devices are 32-bit elements; how exact they have to be, the bound alone decides.
A program may use at most 128 MiB of HBM per device.

```python
import jax
import jax.numpy as jnp
from jax import lax

TILE = 128
SLOTS = 2
FINE_DEV = 32
GROUPS = 16
FINE_GRP = 512
BLOCKS = 8192
COARSE_GRP = 512
CTILES = 4
N_DEV = 16


def draw_a_tiles(key, part):
    first_key = jax.random.fold_in(key, 0)
    full_shape = (BLOCKS, 3, TILE, TILE)
    noise = jnp.clip(jax.random.normal(first_key, full_shape, jnp.float32), -4.0, 4.0)
    rising = 1.0 + 2.0 * jnp.arange(BLOCKS, dtype=jnp.float32) / max(BLOCKS - 1, 1)
    diag_coef = jnp.where(jnp.arange(3)[None, :] == 1, 6.0 * rising[:, None], -1.0)
    return noise * (2.0 / TILE ** 0.5) + diag_coef[:, :, None, None] * jnp.eye(TILE, dtype=jnp.float32)


def draw_coarse_ids(key, part):
    favor_key = jax.random.fold_in(key, 11)
    roll_key = jax.random.fold_in(key, 12)
    other_key = jax.random.fold_in(key, 13)
    second_key = jax.random.fold_in(key, 14)
    block_index = jnp.arange(BLOCKS, dtype=jnp.int32)
    group_of = block_index // FINE_GRP
    local_dev = block_index % FINE_GRP // FINE_DEV
    dev_total = FINE_GRP // FINE_DEV
    favored = jax.random.randint(favor_key, (GROUPS,), 0, CTILES, dtype=jnp.int32)[group_of]
    threshold = 20 + 70 * local_dev // max(dev_total - 1, 1)
    rolled = jax.random.randint(roll_key, (BLOCKS,), 0, 100, dtype=jnp.int32)
    other = jax.random.randint(other_key, (BLOCKS,), 0, CTILES, dtype=jnp.int32)
    first = jnp.where(rolled < threshold, favored, other)
    offset = jax.random.randint(second_key, (BLOCKS,), 0, CTILES - 1, dtype=jnp.int32)
    second = (first + 1 + offset) % CTILES
    return jnp.stack([first, second], axis=1).astype(jnp.int32)


def shard_levels(own_key, dims, pieces, least, top_value):
    factor_of, own = 1.0, jax.random.fold_in(own_key, 6)
    for dim, parts in pieces:
        draws = jnp.exp(jax.random.uniform(jax.random.fold_in(own, dim), (parts,), jnp.float32, least / len(pieces), top_value / len(pieces)))
        factor_of = factor_of * jnp.repeat(draws, dims[dim] // parts).reshape([-1 if axis == dim else 1 for axis in range(len(dims))])
    return factor_of


def gaussian(stream_key, extent, scale, bound, cuts=(), kind=jnp.bfloat16):
    entries = jax.random.normal(stream_key, extent, jnp.float32) * scale
    if len(cuts) > 0:
        entries = shard_levels(stream_key, extent, cuts, -0.22, 0.18) * entries
    return jnp.clip(entries, min=-bound, max=bound).astype(kind)


def setup_inputs(seed: int = 0) -> dict:
    splits = jax.random.split(jax.random.key(seed), 4)
    return {
        "a_tiles": draw_a_tiles(jax.random.fold_in(splits[3], 71), 0),
        "prolong": gaussian(splits[1], (BLOCKS, SLOTS, TILE, TILE), TILE ** -0.5, 0.5, ((0, 256),), jnp.float32),
        "coarse_ids": draw_coarse_ids(jax.random.fold_in(splits[3], 71), 0),
    }


def coarse_tiles(own_a, nearby):
    block_count = own_a.shape[0]
    slot_count = nearby.shape[1]
    tile_size = nearby.shape[2]
    widened = jnp.transpose(nearby, (0, 2, 1, 3)).reshape(block_count + 2, tile_size, slot_count * tile_size)
    stacked = jnp.stack([widened[:-2], widened[1:-1], widened[2:]], axis=1)
    right_prod = jnp.einsum("bnij,bnjk->bnik", own_a, stacked, precision=lax.Precision.HIGHEST)
    right_prod = jnp.transpose(right_prod, (0, 2, 1, 3)).reshape(block_count, tile_size, 3 * slot_count * tile_size)
    left_prod = jnp.einsum("bik,bic->bkc", widened[1:-1], right_prod, precision=lax.Precision.HIGHEST)
    left_prod = left_prod.reshape(block_count, slot_count, tile_size, 3 * slot_count, tile_size)
    return jnp.transpose(left_prod, (0, 1, 3, 2, 4))


def reference(a_tiles, prolong, coarse_ids):
    block_index = jnp.arange(BLOCKS, dtype=jnp.int32)
    group_of = block_index // FINE_GRP
    within = block_index % FINE_GRP
    lower_win = jnp.where(within == 0, 0, 1).astype(jnp.int32)
    upper_win = jnp.where(within == FINE_GRP - 1, 2, 1).astype(jnp.int32)
    prev_ids = jnp.roll(coarse_ids, 1, axis=0)
    next_ids = jnp.roll(coarse_ids, -1, axis=0)
    row_tiles = group_of[:, None] * CTILES + coarse_ids
    col_tiles = jnp.concatenate([lower_win[:, None] * CTILES + prev_ids, CTILES + coarse_ids, upper_win[:, None] * CTILES + next_ids], axis=1)

    def add_batch(batch_index, raw_tiles):
        first_block = (batch_index * FINE_DEV).astype(jnp.int32)
        picked = (first_block - 1 + jnp.arange(FINE_DEV + 2, dtype=jnp.int32)) % BLOCKS
        nearby = jnp.take(prolong, picked, axis=0)
        own_a = lax.dynamic_slice_in_dim(a_tiles, first_block, FINE_DEV, 0)
        rows_here = lax.dynamic_slice_in_dim(row_tiles, first_block, FINE_DEV, 0)
        cols_here = lax.dynamic_slice_in_dim(col_tiles, first_block, FINE_DEV, 0)
        products = coarse_tiles(own_a, nearby)
        return raw_tiles.at[rows_here[:, :, None], cols_here[:, None, :]].add(products)

    raw_start = jnp.zeros((GROUPS * CTILES, 3 * CTILES, TILE, TILE), jnp.float32)
    raw_tiles = lax.fori_loop(0, GROUPS * N_DEV, add_batch, raw_start)
    tile_index = jnp.arange(GROUPS * CTILES, dtype=jnp.int32)
    diag_tiles = raw_tiles[tile_index, CTILES + tile_index % CTILES]
    mean_diag = jnp.sum(jnp.diagonal(diag_tiles, axis1=1, axis2=2)) / (GROUPS * COARSE_GRP)
    coarse = jnp.transpose(raw_tiles / mean_diag, (0, 2, 1, 3)).reshape(GROUPS * COARSE_GRP, 3 * COARSE_GRP)
    return coarse
```

```python
import jax
import jax.numpy as jnp
from jax import lax
from jax.experimental import pallas as pl
from jax.experimental.pallas import tpu as pltpu
from jax.sharding import Mesh
from jax.sharding import PartitionSpec as P

GRP_DEV = ("grp_0", "grp_1", "grp_2", "dev_0", "dev_1")
AXES = GRP_DEV
NB = 32
T = 128
CT = 4
PZ = 192
F32 = jnp.float32
BF16 = jnp.bfloat16


def coords(index):
    grp, dev = index // 16, index % 16
    return (grp // 4, grp // 2 % 2, grp % 2, dev // 4, dev % 4)


def split(x):
    hi = x.astype(BF16)
    lo = (x - hi.astype(F32)).astype(BF16)
    return hi, lo


def twice(x):
    return jnp.concatenate([x, x], axis=1)


def kernel(
    ids,
    a_hbm,
    p_hbm,
    out,
    a_buf,
    p_buf,
    pt,
    prod,
    r2,
    halo,
    halo_id,
    id_send,
    c_send,
    y_a,
    y_b,
    y_d,
    z_send,
    z_recv,
    e_send,
    e_recv,
    t_send,
    t_one,
    t_two,
    sem_a,
    sem_p,
    sem_hs,
    sem_hr,
    sem_ys,
    sem_yr,
    sem_zs,
    sem_zr,
    sem_es,
    sem_er,
    sem_ts,
    sem_tr,
):
    gx, gz, gc, dz, dy = (lax.axis_index(name) for name in AXES)
    grp = gx * 4 + gz * 2 + gc
    dev = dz * 4 + dy
    me = grp * 16 + dev

    def dev_peer(rel):
        other = lax.rem(dev + rel, 16)
        return (gx, gz, gc, other // 4, lax.rem(other, 4))

    def grp_peer(rel):
        other = lax.rem(grp + rel, 16)
        return (other // 4, lax.rem(other // 2, 2), lax.rem(other, 2), dz, dy)

    def y_peer(rel):
        return (gx, gz, gc, dz, lax.rem(dy + rel, 4))

    def z_peer(rel):
        return (gx, gz, gc, lax.rem(dz + rel, 4), dy)

    def ring_peer(rel):
        other = lax.rem(me + rel, 256)
        g, d = other // 16, lax.rem(other, 16)
        return (g // 4, lax.rem(g // 2, 2), lax.rem(g, 2), d // 4, lax.rem(d, 4))

    nxt, prv = ring_peer(1), ring_peer(255)
    barrier = pltpu.get_barrier_semaphore()
    for peer in [nxt, prv] + [dev_peer(k) for k in range(1, 16)] + [grp_peer(k) for k in range(1, 16)]:
        pl.semaphore_signal(barrier, inc=1, device_id=peer, device_id_type=pl.DeviceIdType.MESH)

    def remote(src, dst, send, recv, peer):
        return pltpu.make_async_remote_copy(
            src_ref=src,
            dst_ref=dst,
            send_sem=send,
            recv_sem=recv,
            device_id=peer,
            device_id_type=pl.DeviceIdType.MESH,
        )

    def load_a(g):
        cut = pl.ds(g * 4, 4)
        return pltpu.make_async_copy(a_hbm.at[cut], a_buf.at[cut], sem_a.at[g])

    def load_p(g):
        cut = pl.ds(g * 4, 4)
        return pltpu.make_async_copy(p_hbm.at[cut], p_buf.at[cut], sem_p.at[g])

    load_p(0).start()
    load_a(0).start()
    load_a(1).start()
    load_p(7).start()
    for g in range(1, 7):
        load_p(g).start()
        load_a(g + 1).start()

    zero_f = jnp.zeros((T, T), F32)
    zero_b = jnp.zeros((T, T), BF16)
    prod[PZ] = zero_f
    pt[64] = zero_b
    pt[129] = zero_b
    for side, block in ((0, 0), (1, NB - 1)):
        for slot in range(2):
            id_send[side, :, slot * T : (slot + 1) * T] = jnp.full((8, T), ids[block, slot], jnp.int32)

    def pick(block, j, first, none):
        return jnp.where(ids[block, 0] == j, first, jnp.where(ids[block, 1] == j, first + 1, none))

    def push_p(p0, p1, unit):
        h0, l0 = split(p0)
        h1, l1 = split(p1)
        high, low = jnp.concatenate([h0, h1], axis=1), jnp.concatenate([l0, l1], axis=1)
        pltpu.matmul_push_rhs(jnp.concatenate([high, low], axis=0), 0, unit)
        return (h0, h1), (l0, l1)

    def gather(n0, n1, n2, j, ends):
        total = prod[pick(n1, j, n1 * 6 + 2, PZ)]
        if ends != 0:
            total = total + prod[pick(n0, j, n0 * 6, PZ)]
        if ends != 1:
            total = total + prod[pick(n2, j, n2 * 6 + 4, PZ)]
        return total

    def put_r(pair, half, j, value):
        hi, lo = split(value)
        r2[pair, 0, half * T : (half + 1) * T, j * T : (j + 1) * T] = hi
        r2[pair, 1, half * T : (half + 1) * T, j * T : (j + 1) * T] = lo

    def assemble(pair):
        for half in range(2):
            block = pair * 2 - 1 + half
            low = jnp.maximum(block - 1, 0)
            mid = jnp.maximum(block, 0)
            for j in range(CT):
                put_r(pair, half, j, gather(low, mid, block + 1, j, None))

    def body(acc0, acc1, tot):
        acc = (acc0, acc1)

        def products(t):
            for unit in range(2):
                n = t * 2 + unit
                high, low = push_p(p_buf[n, 0], p_buf[n, 1], unit)
                for slot in range(2):
                    pt[n * 2 + slot] = high[slot].T
                    pt[65 + n * 2 + slot] = low[slot].T
                for m in range(3):
                    hi, lo = split(a_buf[jnp.clip(n + 1 - m, 0, NB - 1), m])
                    pltpu.matmul_acc_lhs(acc[unit][m], twice(hi), load_staged_rhs=0 if m == 0 else None)
                    pltpu.matmul_acc_lhs(acc[unit][m], twice(lo))

        def drain(t):
            for unit in range(2):
                n = t * 2 + unit
                for m in range(3):
                    res = pltpu.matmul_pop(acc[unit][m])
                    prod[(n * 3 + m) * 2] = res[:, :T]
                    prod[(n * 3 + m) * 2 + 1] = res[:, T:]

        def step(t):
            products(t)
            assemble(jnp.maximum(t - 1, 0))
            drain(t)

        def one_group(g, carry):
            load_p(g).wait()

            @pl.when(g < 7)
            def _():
                load_a(g + 1).wait()

            step(g * 2)
            step(g * 2 + 1)
            return carry

        load_p(0).wait()
        load_a(0).wait()
        load_a(1).wait()
        step(0)
        step(1)
        load_p(7).wait()

        pl.semaphore_wait(barrier, 32)
        halo_copies = [
            remote(p_buf.at[NB - 1], halo.at[0], sem_hs.at[0], sem_hr.at[0], nxt),
            remote(p_buf.at[0], halo.at[1], sem_hs.at[1], sem_hr.at[1], prv),
            remote(id_send.at[1], halo_id.at[0], sem_hs.at[2], sem_hr.at[2], nxt),
            remote(id_send.at[0], halo_id.at[1], sem_hs.at[3], sem_hr.at[3], prv),
        ]
        for copy in halo_copies:
            copy.start()

        def later_group(g, carry):
            load_p(g).wait()
            load_a(g + 1).wait()
            step(g * 2)
            step(g * 2 + 1)
            return carry

        lax.fori_loop(1, 7, later_group, 0)
        step(14)
        step(15)
        assemble(15)

        for copy in halo_copies:
            copy.wait_recv()
        for side in range(2):
            push_p(halo[side, 0], halo[side, 1], side)
            hi, lo = split(a_buf[0, 0] if side == 0 else a_buf[NB - 1, 2])
            pltpu.matmul_acc_lhs(acc[side][0], twice(hi), load_staged_rhs=0)
            pltpu.matmul_acc_lhs(acc[side][0], twice(lo))
        edge = [pltpu.matmul_pop(acc[side][0]) for side in range(2)]
        for side in range(2):
            prod[193 + side * 2] = edge[side][:, :T]
            prod[194 + side * 2] = edge[side][:, T:]
        inner = [dev > 0, dev < 15]
        for half, side in ((0, 1), (1, 0)):
            for j in range(CT):
                own = gather(30, 31, 31, j, 1) if side == 1 else gather(0, 0, 1, j, 0)
                extra = zero_f
                for slot in range(2):
                    match = halo_id[side, 0:1, slot * T : (slot + 1) * T] == j
                    extra = extra + jnp.where(match, prod[193 + side * 2 + slot], 0.0)
                put_r(0, half, j, own + jnp.where(inner[side], extra, 0.0))

        def lhs(b0, b1, i, low):
            base = 65 if low else 0
            none = 129 if low else 64
            return jnp.concatenate(
                [pt[pick(b0, i, base + b0 * 2, none)], pt[pick(b1, i, base + b1 * 2, none)]], axis=1
            )

        for side, at in ((0, 0), (1, 15)):

            @pl.when(dev == at)
            def _(side=side):
                block = 0 if side == 0 else NB - 1
                y0, y1 = prod[193 + side * 2], prod[194 + side * 2]
                h0, l0 = split(y0)
                h1, l1 = split(y1)
                for part, (q0, q1) in enumerate(((h0, h1), (l0, l1))):
                    row = jnp.concatenate([q0, q1], axis=1)
                    for unit in range(2):
                        pltpu.matmul_push_rhs(jnp.concatenate([row, row], axis=0), 0, unit)
                        left = [
                            jnp.concatenate(
                                [pt[pick(block, i, block * 2, 64)], pt[pick(block, i, 65 + block * 2, 129)]], axis=1
                            )
                            for i in (unit * 2, unit * 2 + 1)
                        ]
                        pltpu.matmul_acc_lhs(tot[unit], jnp.concatenate(left, axis=0), load_staged_rhs=0)
                for unit in range(2):
                    res = pltpu.matmul_pop(tot[unit])
                    for k in range(8):
                        e_send[side, unit * 8 + k, 0:32] = res[k * 32 : (k + 1) * 32]
                code = halo_id[side].astype(F32)
                for k in range(16):
                    e_send[side, k, 32:40] = code
                for rel in range(1, 16):
                    other = lax.rem(dev + rel, 16)
                    remote(
                        e_send.at[side, other], e_recv.at[side], sem_es.at[side, rel], sem_er.at[side], dev_peer(rel)
                    ).start()
                e_recv[side] = e_send[side, at]

        def totals(chunk):
            columns = slice(chunk * 2 * T, (chunk + 1) * 2 * T)

            def pair_step(pair, b0, b1):
                for unit in range(2):
                    rows = (unit * 2, unit * 2 + 1)
                    high = jnp.concatenate([lhs(b0, b1, i, False) for i in rows], axis=0)
                    low = jnp.concatenate([lhs(b0, b1, i, True) for i in rows], axis=0)
                    pltpu.matmul_push_rhs(r2[pair, 0, :, columns], 0, unit)
                    pltpu.matmul_push_rhs(r2[pair, 1, :, columns], 1, unit)
                    pltpu.matmul_acc_lhs(tot[unit], high, load_staged_rhs=0)
                    pltpu.matmul_acc_lhs(tot[unit], low)
                    pltpu.matmul_acc_lhs(tot[unit], high, load_staged_rhs=1)

            def three(k, carry):
                for u in range(3):
                    pair = k * 3 + 1 + u
                    pair_step(pair, pair * 2 - 1, pair * 2)
                return carry

            lax.fori_loop(0, 5, three, 0)
            pair_step(0, NB - 1, 0)
            eye = (
                lax.broadcasted_iota(jnp.int32, (T, T), 0) == lax.broadcasted_iota(jnp.int32, (T, T), 1)
            )
            diag = jnp.zeros((8, T), F32)
            for unit in range(2):
                res = pltpu.matmul_pop(tot[unit])
                for half in range(2):
                    i = unit * 2 + half
                    for y in range(4):
                        c_send[chunk, y, i] = res[half * T + y * 32 : half * T + (y + 1) * 32]
                if unit == chunk:
                    for half in range(2):
                        tile = jnp.where(eye, res[half * T : (half + 1) * T, half * T : (half + 1) * T], 0.0)
                        diag = diag + jnp.sum(tile.reshape(16, 8, T), axis=0)
            return diag

        up, down = lax.rem(dy + 1, 4), lax.rem(dy + 3, 4)
        far = lax.rem(dy + 2, 4)
        lo2, hi2 = pl.ds(0, 2), pl.ds(2, 2)

        def y_first(c):
            return [
                remote(c_send.at[c, far, lo2], y_a.at[c, 0], sem_ys.at[c, 0], sem_yr.at[c, 0], y_peer(1)),
                remote(c_send.at[c, far, hi2], y_a.at[c, 1], sem_ys.at[c, 1], sem_yr.at[c, 1], y_peer(3)),
                remote(c_send.at[c, up, hi2], y_d.at[c, 0], sem_ys.at[c, 2], sem_yr.at[c, 2], y_peer(1)),
                remote(c_send.at[c, down, lo2], y_d.at[c, 1], sem_ys.at[c, 3], sem_yr.at[c, 3], y_peer(3)),
            ]

        def y_second(c):
            return [
                remote(c_send.at[c, up, lo2], y_b.at[c, 0], sem_ys.at[c, 4], sem_yr.at[c, 4], y_peer(1)),
                remote(c_send.at[c, down, hi2], y_b.at[c, 1], sem_ys.at[c, 5], sem_yr.at[c, 5], y_peer(3)),
            ]

        def z_all(c):
            return [
                remote(
                    z_send.at[c, lax.rem(dz + rel, 4)],
                    z_recv.at[c, rel - 1],
                    sem_zs.at[c, rel - 1],
                    sem_zr.at[c, rel - 1],
                    z_peer(rel),
                )
                for rel in range(1, 4)
            ]

        def begin_second(c):
            first = y_first(c)
            first[0].wait_recv()
            c_send[c, up, lo2] = c_send[c, up, lo2] + y_a[c, 0]
            y_second(c)[0].start()
            first[1].wait_recv()
            c_send[c, down, hi2] = c_send[c, down, hi2] + y_a[c, 1]
            y_second(c)[1].start()

        def begin_z(c):
            for copy in y_first(c)[2:] + y_second(c):
                copy.wait_recv()
            z_send[c, 0:2] = c_send[c, dy, lo2] + y_b[c, 0] + y_d[c, 1]
            z_send[c, 2:4] = c_send[c, dy, hi2] + y_b[c, 1] + y_d[c, 0]
            for copy in z_all(c):
                copy.start()

        diag = totals(0)
        for copy in y_first(0):
            copy.start()
        diag = diag + totals(1)
        t_send[0] = diag

        def t_copies(phase):
            into = t_one if phase == 0 else t_two
            peer = dev_peer if phase == 0 else grp_peer
            return [
                remote(t_send.at[phase], into.at[rel], sem_ts.at[phase, rel], sem_tr.at[phase, rel], peer(rel))
                for rel in range(1, 16)
            ]

        one, two = t_copies(0), t_copies(1)
        for copy in one:
            copy.start()
        for copy in y_first(1):
            copy.start()
        begin_second(0)
        begin_second(1)
        begin_z(0)
        begin_z(1)
        total = diag
        for rel in range(1, 16):
            one[rel - 1].wait_recv()
            total = total + t_one[rel]
        t_send[1] = total
        for copy in two:
            copy.start()
        for rel in range(1, 16):
            two[rel - 1].wait_recv()
            total = total + t_two[rel]
        mean = jnp.sum(total, axis=(0, 1), keepdims=True) * (1.0 / 8192.0)
        scale = jnp.broadcast_to(mean, (32, 2 * T))

        for side, at in ((0, 0), (1, 15)):
            base = 0 if side == 0 else 1024

            @pl.when(dev != at)
            def _(side=side):
                remote(
                    e_send.at[side, 0], e_recv.at[side], sem_es.at[side, 0], sem_er.at[side], dev_peer(1)
                ).wait_recv()

            for j in range(CT):
                value = jnp.zeros((32, T), F32)
                for slot in range(2):
                    match = e_recv[side, 32:33, slot * T : (slot + 1) * T] == float(j)
                    value = value + jnp.where(match, e_recv[side, 0:32, slot * T : (slot + 1) * T], 0.0)
                out[:, base + j * T : base + (j + 1) * T] = value / scale[:, :T]

        for c in range(2):
            value = z_send[c, dz]
            for k, copy in enumerate(z_all(c)):
                copy.wait_recv()
                value = value + z_recv[c, k]
            out[:, 512 + c * 256 : 512 + (c + 1) * 256] = value / scale

        for copy in halo_copies + one + two:
            copy.wait_send()
        for c in range(2):
            for copy in y_first(c) + y_second(c) + z_all(c):
                copy.wait_send()
        for side, at in ((0, 0), (1, 15)):

            @pl.when(dev == at)
            def _(side=side):
                for rel in range(1, 16):
                    remote(
                        e_send.at[side, 0], e_recv.at[side], sem_es.at[side, rel], sem_er.at[side], dev_peer(rel)
                    ).wait_send()

    small = tuple(tuple(pltpu.ACC(unit)((T, 2 * T), F32) for _ in range(3)) for unit in range(2))
    large = tuple(pltpu.ACC(unit)((2 * T, 2 * T), F32) for unit in range(2))
    pl.run_scoped(body, small[0], small[1], large)


def local(a_tiles, prolong, coarse_ids):
    vmem, dma = pltpu.VMEM, pltpu.SemaphoreType.DMA
    return pl.pallas_call(
        kernel,
        out_shape=jax.ShapeDtypeStruct((32, 1536), F32),
        in_specs=[
            pl.BlockSpec(memory_space=pltpu.SMEM),
            pl.BlockSpec(memory_space=pl.ANY),
            pl.BlockSpec(memory_space=pl.ANY),
        ],
        out_specs=pl.BlockSpec(memory_space=pltpu.VMEM),
        scratch_shapes=[
            vmem((NB, 3, T, T), F32),
            vmem((NB, 2, T, T), F32),
            vmem((130, T, T), BF16),
            vmem((197, T, T), F32),
            vmem((16, 2, 2 * T, 4 * T), BF16),
            vmem((2, 2, T, T), F32),
            vmem((2, 8, 2 * T), jnp.int32),
            vmem((2, 8, 2 * T), jnp.int32),
            vmem((2, 4, 4, 32, 2 * T), F32),
            vmem((2, 2, 2, 32, 2 * T), F32),
            vmem((2, 2, 2, 32, 2 * T), F32),
            vmem((2, 2, 2, 32, 2 * T), F32),
            vmem((2, 4, 32, 2 * T), F32),
            vmem((2, 3, 32, 2 * T), F32),
            vmem((2, 16, 40, 2 * T), F32),
            vmem((2, 40, 2 * T), F32),
            vmem((2, 8, T), F32),
            vmem((16, 8, T), F32),
            vmem((16, 8, T), F32),
            dma((8,)),
            dma((8,)),
            dma((4,)),
            dma((4,)),
            dma((2, 6)),
            dma((2, 6)),
            dma((2, 3)),
            dma((2, 3)),
            dma((2, 16)),
            dma((2,)),
            dma((2, 16)),
            dma((2, 16)),
        ],
        compiler_params=pltpu.CompilerParams(
            collective_id=0, has_side_effects=True, vmem_limit_bytes=60 * 1024 * 1024
        ),
    )(coarse_ids, a_tiles, prolong)


def solution(mesh):
    torus = Mesh(mesh.devices.reshape(4, 2, 2, 4, 4), GRP_DEV)

    def run(a_tiles, prolong, coarse_ids):
        return jax.shard_map(
            local,
            mesh=torus,
            in_specs=(P(GRP_DEV, None, None, None), P(GRP_DEV, None, None, None), P(GRP_DEV, None)),
            out_specs=P(GRP_DEV, None),
            check_vma=False,
        )(a_tiles, prolong, coarse_ids)

    return run
```

```python
import jax
import jax.numpy as jnp
from jax import lax
from jax.experimental import pallas as pl
from jax.experimental.pallas import tpu as pltpu
from jax.sharding import Mesh
from jax.sharding import PartitionSpec as P

GRP_DEV = ("grp_0", "grp_1", "grp_2", "dev_0", "dev_1")
AXES = GRP_DEV
NB = 32
T = 128
CT = 4
PZ = 192
VMEM_MIB = 53
F32 = jnp.float32
BF16 = jnp.bfloat16


def coords(index):
    grp, dev = index // 16, index % 16
    return (grp // 4, grp // 2 % 2, grp % 2, dev // 4, dev % 4)


def split(x):
    hi = x.astype(BF16)
    lo = (x - hi.astype(F32)).astype(BF16)
    return hi, lo


def rest(x):
    return x - x.astype(BF16).astype(F32)


def twice(x):
    return jnp.concatenate([x, x], axis=1)


def kernel(
    ids,
    a_hbm,
    p_hbm,
    out,
    a_buf,
    p_buf,
    pt,
    prod,
    r2,
    halo,
    halo_id,
    id_send,
    c_send,
    y_a,
    y_b,
    y_d,
    z_send,
    z_a,
    z_b,
    z_d,
    e_send,
    e_y,
    e_pass,
    e_recv,
    t_send,
    t_one,
    t_two,
    sem_a,
    sem_p,
    sem_hs,
    sem_hr,
    sem_ys,
    sem_yr,
    sem_zs,
    sem_zr,
    sem_es,
    sem_er,
    sem_ts,
    sem_tr,
):
    gx, gz, gc, dz, dy = (lax.axis_index(name) for name in AXES)
    grp = gx * 4 + gz * 2 + gc
    dev = dz * 4 + dy
    me = grp * 16 + dev

    def dev_peer(rel):
        other = lax.rem(dev + rel, 16)
        return (gx, gz, gc, other // 4, lax.rem(other, 4))

    def grp_peer(rel):
        other = lax.rem(grp + rel, 16)
        return (other // 4, lax.rem(other // 2, 2), lax.rem(other, 2), dz, dy)

    def y_peer(rel):
        return (gx, gz, gc, dz, lax.rem(dy + rel, 4))

    def z_peer(rel):
        return (gx, gz, gc, lax.rem(dz + rel, 4), dy)

    def ring_peer(rel):
        other = lax.rem(me + rel, 256)
        g, d = other // 16, lax.rem(other, 16)
        return (g // 4, lax.rem(g // 2, 2), lax.rem(g, 2), d // 4, lax.rem(d, 4))

    def remote(src, dst, send, recv, peer):
        return pltpu.make_async_remote_copy(
            src_ref=src,
            dst_ref=dst,
            send_sem=send,
            recv_sem=recv,
            device_id=peer,
            device_id_type=pl.DeviceIdType.MESH,
        )

    def load_a(g):
        cut = pl.ds(g * 4, 4)
        return pltpu.make_async_copy(a_hbm.at[cut], a_buf.at[cut], sem_a.at[g])

    def load_p(g):
        cut = pl.ds(g * 8, 8)
        return pltpu.make_async_copy(p_hbm.at[cut], p_buf.at[cut], sem_p.at[g])

    load_p(0).start()
    load_a(0).start()
    load_a(1).start()
    load_p(7).start()
    for g in range(1, 7):
        load_p(g).start()
        load_a(g + 1).start()

    nxt, prv = ring_peer(1), ring_peer(255)
    barrier = pltpu.get_barrier_semaphore()
    with jax.named_scope("signals"):
        for peer in [nxt, prv] + [dev_peer(k) for k in range(1, 16)] + [grp_peer(k) for k in range(1, 16)]:
            pl.semaphore_signal(barrier, inc=1, device_id=peer, device_id_type=pl.DeviceIdType.MESH)

    zero_f = jnp.zeros((T, T), F32)
    zero_b = jnp.zeros((T, T), BF16)
    prod[PZ] = zero_f
    p_buf[64] = zero_f
    pt[64] = zero_b
    pt[129] = zero_b
    for side, block in ((0, 0), (1, NB - 1)):
        for slot in range(2):
            id_send[side, :, slot * T : (slot + 1) * T] = jnp.full((8, T), ids[slot, block], jnp.int32)

    def pick(block, j, first, none):
        return jnp.where(ids[0, block] == j, first, jnp.where(ids[1, block] == j, first + 1, none))

    def push_p(p0, p1, unit):
        h0, l0 = split(p0)
        h1, l1 = split(p1)
        high, low = jnp.concatenate([h0, h1], axis=1), jnp.concatenate([l0, l1], axis=1)
        pltpu.matmul_push_rhs(jnp.concatenate([high, low], axis=0), 0, unit)
        return (h0, h1), (l0, l1)

    def gather(n0, n1, n2, j, ends):
        total = prod[pick(n1, j, n1 * 6 + 2, PZ)]
        if ends != 0:
            total = total + prod[pick(n0, j, n0 * 6, PZ)]
        if ends != 1:
            total = total + prod[pick(n2, j, n2 * 6 + 4, PZ)]
        return total

    def put_r(pair, half, j, value):
        r2[pair, 0, j, half * T : (half + 1) * T] = value
        r2[pair, 1, j, half * T : (half + 1) * T] = rest(value)

    def assemble(pair):
        for half in range(2):
            block = pair * 2 - 1 + half
            low = jnp.maximum(block - 1, 0)
            mid = jnp.maximum(block, 0)
            for j in range(CT):
                put_r(pair, half, j, gather(low, mid, block + 1, j, None))

    def body(acc, odd, tot):

        def products(t, into):
            for unit in range(2):
                n = t * 2 + unit
                high, low = push_p(p_buf[n * 2], p_buf[n * 2 + 1], unit)
                for slot in range(2):
                    pt[n * 2 + slot] = high[slot].T
                    pt[65 + n * 2 + slot] = low[slot].T
                for m in range(3):
                    tile = a_buf[jnp.clip(n + 1 - m, 0, NB - 1), m]
                    pltpu.matmul_acc_lhs(into[unit][m], twice(tile), load_staged_rhs=0 if m == 0 else None)
                    pltpu.matmul_acc_lhs(into[unit][m], twice(rest(tile)))

        def drain(t, into):
            for unit in range(2):
                n = t * 2 + unit
                for m in range(3):
                    res = pltpu.matmul_pop(into[unit][m])
                    prod[(n * 3 + m) * 2] = res[:, :T]
                    prod[(n * 3 + m) * 2 + 1] = res[:, T:]

        def steps(t):
            products(t, acc)
            products(t + 1, odd)
            assemble(jnp.maximum(t - 1, 0))
            drain(t, acc)
            assemble(t)
            drain(t + 1, odd)

        with jax.named_scope("load"):
            load_p(0).wait()
            load_a(0).wait()
            load_a(1).wait()
        with jax.named_scope("two_steps"):
            steps(0)
        with jax.named_scope("load7"):
            load_p(7).wait()
        with jax.named_scope("barrier"):
            pl.semaphore_wait(barrier, 32)
        halo_copies = [
            remote(p_buf.at[pl.ds(62, 2)], halo.at[0], sem_hs.at[0], sem_hr.at[0], nxt),
            remote(p_buf.at[pl.ds(0, 2)], halo.at[1], sem_hs.at[1], sem_hr.at[1], prv),
            remote(id_send.at[1], halo_id.at[0], sem_hs.at[2], sem_hr.at[2], nxt),
            remote(id_send.at[0], halo_id.at[1], sem_hs.at[3], sem_hr.at[3], prv),
        ]
        for copy in halo_copies:
            copy.start()

        def later_group(g, carry):
            load_p(g).wait()
            load_a(g + 1).wait()
            steps(g * 2)
            return carry

        with jax.named_scope("right_loop"):
            lax.fori_loop(1, 7, later_group, 0)
        with jax.named_scope("right_end"):
            steps(14)
            assemble(15)

        with jax.named_scope("halo_wait"):
            for copy in halo_copies:
                copy.wait_recv()
        for side in range(2):
            push_p(halo[side, 0], halo[side, 1], side)
            tile = a_buf[0, 0] if side == 0 else a_buf[NB - 1, 2]
            pltpu.matmul_acc_lhs(acc[side][0], twice(tile), load_staged_rhs=0)
            pltpu.matmul_acc_lhs(acc[side][0], twice(rest(tile)))
        edge = [pltpu.matmul_pop(acc[side][0]) for side in range(2)]
        for side in range(2):
            prod[193 + side * 2] = edge[side][:, :T]
            prod[194 + side * 2] = edge[side][:, T:]
        inner = [dev > 0, dev < 15]
        for half, side in ((0, 1), (1, 0)):
            for j in range(CT):
                own = gather(30, 31, 31, j, 1) if side == 1 else gather(0, 0, 1, j, 0)
                extra = zero_f
                for slot in range(2):
                    match = halo_id[side, 0:1, slot * T : (slot + 1) * T] == j
                    extra = extra + jnp.where(match, prod[193 + side * 2 + slot], 0.0)
                put_r(0, half, j, own + jnp.where(inner[side], extra, 0.0))

        def lhs(b0, b1, i, low):
            base = 65 if low else 0
            none = 129 if low else 64
            return jnp.concatenate(
                [pt[pick(b0, i, base + b0 * 2, none)], pt[pick(b1, i, base + b1 * 2, none)]], axis=1
            )

        ends = ((0, 0), (1, 15))

        def edge_y(side, rel):
            other = lax.rem(dy + rel, 4)
            return remote(
                e_send.at[side, other], e_y.at[side], sem_es.at[side, rel - 1], sem_er.at[side, 0], y_peer(rel)
            )

        def edge_z(side, rel):
            other = lax.rem(dz + rel, 4)
            return remote(
                e_pass.at[side, other], e_recv.at[side], sem_es.at[side, rel + 2], sem_er.at[side, 1], z_peer(rel)
            )

        for side, at in ends:

            @pl.when(dev == at)
            def _(side=side, at=at):
                block = 0 if side == 0 else NB - 1
                y0, y1 = prod[193 + side * 2], prod[194 + side * 2]
                wide = jnp.concatenate([y0, y1], axis=1)
                for part in (wide, rest(wide)):
                    for unit in range(2):
                        pltpu.matmul_push_rhs(jnp.concatenate([part, part], axis=0), 0, unit)
                        left = jnp.concatenate([pt[block * 2 + unit], pt[65 + block * 2 + unit]], axis=1)
                        pltpu.matmul_acc_lhs(acc[unit][0], left, load_staged_rhs=0)
                for unit in range(2):
                    res = pltpu.matmul_pop(acc[unit][0])
                    for y in range(4):
                        e_send[side, y, unit * 32 : (unit + 1) * 32] = res[y * 32 : (y + 1) * 32]
                upper = lax.broadcasted_iota(jnp.int32, (8, 2 * T), 0) < 4
                code = jnp.where(upper, halo_id[side], id_send[side]).astype(F32)
                for y in range(4):
                    e_send[side, y, 64:72] = code
                for rel in range(1, 4):
                    edge_y(side, rel).start()
                e_y[side] = e_send[side, at % 4]

        def pass_edges():
            for side, at in ends:

                @pl.when(dz == at // 4)
                def _(side=side, at=at):
                    @pl.when(dy != at % 4)
                    def _():
                        edge_y(side, 1).wait_recv()

                    for z in range(4):
                        for part in range(2):
                            half = slice(part * T, (part + 1) * T)
                            value = jnp.zeros((32, T), F32)
                            for slot in range(2):
                                match = e_y[side, 68:69, slot * T : (slot + 1) * T] == float(z)
                                value = value + jnp.where(match, e_y[side, slot * 32 : (slot + 1) * 32, half], 0.0)
                            e_pass[side, z, 0:32, half] = value
                        e_pass[side, z, 32:40] = e_y[side, 64:72]
                    for rel in range(1, 4):
                        edge_z(side, rel).start()
                    e_recv[side] = e_pass[side, at // 4]

        def totals(chunk, between):
            def right(pair, part):
                return jnp.concatenate([r2[pair, part, chunk * 2], r2[pair, part, chunk * 2 + 1]], axis=1)

            def pair_step(pair, b0, b1):
                for unit in range(2):
                    rows = (unit * 2, unit * 2 + 1)
                    high = jnp.concatenate([lhs(b0, b1, i, False) for i in rows], axis=0)
                    low = jnp.concatenate([lhs(b0, b1, i, True) for i in rows], axis=0)
                    pltpu.matmul_push_rhs(right(pair, 0), 0, unit)
                    pltpu.matmul_push_rhs(right(pair, 1), 1, unit)
                    pltpu.matmul_acc_lhs(tot[unit], high, load_staged_rhs=0)
                    pltpu.matmul_acc_lhs(tot[unit], low)
                    pltpu.matmul_acc_lhs(tot[unit], high, load_staged_rhs=1)

            def dots(pair, b0, b1, total):
                for half, block in ((0, b0), (1, b1)):
                    for j in range(CT):
                        both = r2[pair, 0, j, half * T : (half + 1) * T] * p_buf[pick(block, j, block * 2, 64)]
                        total = total + jnp.sum(both.reshape(16, 8, T), axis=0)
                return total

            def several(k, total):
                for u in range(3):
                    pair = k * 3 + 1 + u
                    pair_step(pair, pair * 2 - 1, pair * 2)
                    if chunk == 0:
                        total = dots(pair, pair * 2 - 1, pair * 2, total)
                return total

            total = jnp.zeros((8, T), F32)
            for k, (first, last) in enumerate(((0, 2), (2, 5))):
                with jax.named_scope("left_loop"):
                    total = lax.fori_loop(first, last, several, total)
                if k == 0:
                    between()
            pair_step(0, NB - 1, 0)
            if chunk == 0:
                total = dots(0, NB - 1, 0, total)
            for unit in range(2):
                res = pltpu.matmul_pop(tot[unit])
                for half in range(2):
                    i = unit * 2 + half
                    for y in range(4):
                        c_send[chunk, y, i] = res[half * T + y * 32 : half * T + (y + 1) * 32]
            return total

        up, down = lax.rem(dy + 1, 4), lax.rem(dy + 3, 4)
        far = lax.rem(dy + 2, 4)
        lo2, hi2 = pl.ds(0, 2), pl.ds(2, 2)

        def y_first(c):
            return [
                remote(c_send.at[c, far, lo2], y_a.at[c, 0], sem_ys.at[c, 0], sem_yr.at[c, 0], y_peer(1)),
                remote(c_send.at[c, far, hi2], y_a.at[c, 1], sem_ys.at[c, 1], sem_yr.at[c, 1], y_peer(3)),
                remote(c_send.at[c, up, hi2], y_d.at[c, 0], sem_ys.at[c, 2], sem_yr.at[c, 2], y_peer(1)),
                remote(c_send.at[c, down, lo2], y_d.at[c, 1], sem_ys.at[c, 3], sem_yr.at[c, 3], y_peer(3)),
            ]

        def y_second(c):
            return [
                remote(c_send.at[c, up, lo2], y_b.at[c, 0], sem_ys.at[c, 4], sem_yr.at[c, 4], y_peer(1)),
                remote(c_send.at[c, down, hi2], y_b.at[c, 1], sem_ys.at[c, 5], sem_yr.at[c, 5], y_peer(3)),
            ]

        z_up, z_down, z_far = lax.rem(dz + 1, 4), lax.rem(dz + 3, 4), lax.rem(dz + 2, 4)
        top, low16 = pl.ds(0, 16), pl.ds(16, 16)

        def z_first(c):
            return [
                remote(z_send.at[c, z_far, top], z_a.at[c, 0], sem_zs.at[c, 0], sem_zr.at[c, 0], z_peer(1)),
                remote(z_send.at[c, z_far, low16], z_a.at[c, 1], sem_zs.at[c, 1], sem_zr.at[c, 1], z_peer(3)),
                remote(z_send.at[c, z_up, low16], z_d.at[c, 0], sem_zs.at[c, 2], sem_zr.at[c, 2], z_peer(1)),
                remote(z_send.at[c, z_down, top], z_d.at[c, 1], sem_zs.at[c, 3], sem_zr.at[c, 3], z_peer(3)),
            ]

        def z_second(c):
            return [
                remote(z_send.at[c, z_up, top], z_b.at[c, 0], sem_zs.at[c, 4], sem_zr.at[c, 4], z_peer(1)),
                remote(z_send.at[c, z_down, low16], z_b.at[c, 1], sem_zs.at[c, 5], sem_zr.at[c, 5], z_peer(3)),
            ]

        def begin_second(c):
            first = y_first(c)
            first[0].wait_recv()
            c_send[c, up, lo2] = c_send[c, up, lo2] + y_a[c, 0]
            y_second(c)[0].start()
            first[1].wait_recv()
            c_send[c, down, hi2] = c_send[c, down, hi2] + y_a[c, 1]
            y_second(c)[1].start()

        def begin_z(c):
            for copy in y_first(c)[2:] + y_second(c):
                copy.wait_recv()
            z_send[c, 0:2] = c_send[c, dy, lo2] + y_b[c, 0] + y_d[c, 1]
            z_send[c, 2:4] = c_send[c, dy, hi2] + y_b[c, 1] + y_d[c, 0]
            for copy in z_first(c):
                copy.start()

        def second_z(c):
            first = z_first(c)
            first[0].wait_recv()
            z_send[c, z_up, top] = z_send[c, z_up, top] + z_a[c, 0]
            z_second(c)[0].start()
            first[1].wait_recv()
            z_send[c, z_down, low16] = z_send[c, z_down, low16] + z_a[c, 1]
            z_second(c)[1].start()

        def t_copies(phase):
            into = t_one if phase == 0 else t_two
            peer = dev_peer if phase == 0 else grp_peer
            return [
                remote(t_send.at[phase], into.at[rel], sem_ts.at[phase, rel], sem_tr.at[phase, rel], peer(rel))
                for rel in range(1, 16)
            ]

        one, two = t_copies(0), t_copies(1)

        def start(copies):
            for copy in copies:
                copy.start()

        total = totals(0, lambda: None)
        t_send[0] = total
        start(y_first(0)[:2])
        start(one)

        def between():
            start(y_first(0)[2:])
            pass_edges()

        totals(1, between)
        start(y_first(1)[:2])
        with jax.named_scope("y_second_0"):
            begin_second(0)
        start(y_first(1)[2:])
        with jax.named_scope("trace_dev"):
            for rel in range(1, 16):
                one[rel - 1].wait_recv()
                total = total + t_one[rel]
            t_send[1] = total
            start(two)
        with jax.named_scope("y_second_1"):
            begin_second(1)
        with jax.named_scope("z_0"):
            begin_z(0)
        with jax.named_scope("z_1"):
            begin_z(1)
        with jax.named_scope("z_second_0"):
            second_z(0)
        with jax.named_scope("z_second_1"):
            second_z(1)
        with jax.named_scope("trace_grp"):
            for rel in range(1, 16):
                two[rel - 1].wait_recv()
                total = total + t_two[rel]
        mean = jnp.sum(total, axis=(0, 1), keepdims=True) * (1.0 / 8192.0)
        scale = jnp.broadcast_to(mean, (32, 2 * T))

        for side, at in ends:
            base = 0 if side == 0 else 1024

            with jax.named_scope("edge_wait"):

                @pl.when(dz != at // 4)
                def _(side=side):
                    edge_z(side, 1).wait_recv()

            for j in range(CT):
                value = jnp.zeros((32, T), F32)
                for slot in range(2):
                    match = e_recv[side, 32:33, slot * T : (slot + 1) * T] == float(j)
                    value = value + jnp.where(match, e_recv[side, 0:32, slot * T : (slot + 1) * T], 0.0)
                out[:, base + j * T : base + (j + 1) * T] = value / scale[:, :T]

        for c in range(2):
            with jax.named_scope("z_wait"):
                for copy in z_first(c)[2:] + z_second(c):
                    copy.wait_recv()
            value = jnp.concatenate(
                [
                    z_send[c, dz, top] + z_b[c, 0] + z_d[c, 1],
                    z_send[c, dz, low16] + z_b[c, 1] + z_d[c, 0],
                ],
                axis=0,
            )
            out[:, 512 + c * 256 : 512 + (c + 1) * 256] = value / scale

        done = jax.named_scope("sends_done")
        done.__enter__()
        for copy in halo_copies + one + two:
            copy.wait_send()
        for c in range(2):
            for copy in y_first(c) + y_second(c) + z_first(c) + z_second(c):
                copy.wait_send()
        for side, at in ends:

            @pl.when(dev == at)
            def _(side=side):
                for rel in range(1, 4):
                    edge_y(side, rel).wait_send()

            @pl.when(dz == at // 4)
            def _(side=side):
                for rel in range(1, 4):
                    edge_z(side, rel).wait_send()

        done.__exit__(None, None, None)

    small, other = (
        tuple(tuple(pltpu.ACC(unit)((T, 2 * T), F32) for _ in range(3)) for unit in range(2)) for _ in range(2)
    )
    large = tuple(pltpu.ACC(unit)((2 * T, 2 * T), F32) for unit in range(2))
    pl.run_scoped(body, small, other, large)


def local(a_tiles, prolong, coarse_ids):
    vmem, dma = pltpu.VMEM, pltpu.SemaphoreType.DMA
    return pl.pallas_call(
        kernel,
        out_shape=jax.ShapeDtypeStruct((32, 1536), F32),
        in_specs=[
            pl.BlockSpec(memory_space=pltpu.SMEM),
            pl.BlockSpec(memory_space=pltpu.HBM),
            pl.BlockSpec(memory_space=pltpu.HBM),
        ],
        out_specs=pl.BlockSpec(memory_space=pltpu.VMEM),
        scratch_shapes=[
            vmem((NB, 3, T, T), F32),
            vmem((65, T, T), F32),
            vmem((130, T, T), BF16),
            vmem((197, T, T), F32),
            vmem((16, 2, 4, 2 * T, T), F32),
            vmem((2, 2, T, T), F32),
            vmem((2, 8, 2 * T), jnp.int32),
            vmem((2, 8, 2 * T), jnp.int32),
            vmem((2, 4, 4, 32, 2 * T), F32),
            vmem((2, 2, 2, 32, 2 * T), F32),
            vmem((2, 2, 2, 32, 2 * T), F32),
            vmem((2, 2, 2, 32, 2 * T), F32),
            vmem((2, 4, 32, 2 * T), F32),
            vmem((2, 2, 16, 2 * T), F32),
            vmem((2, 2, 16, 2 * T), F32),
            vmem((2, 2, 16, 2 * T), F32),
            vmem((2, 4, 72, 2 * T), F32),
            vmem((2, 72, 2 * T), F32),
            vmem((2, 4, 40, 2 * T), F32),
            vmem((2, 40, 2 * T), F32),
            vmem((2, 8, T), F32),
            vmem((16, 8, T), F32),
            vmem((16, 8, T), F32),
            dma((8,)),
            dma((8,)),
            dma((4,)),
            dma((4,)),
            dma((2, 6)),
            dma((2, 6)),
            dma((2, 6)),
            dma((2, 6)),
            dma((2, 6)),
            dma((2, 2)),
            dma((2, 16)),
            dma((2, 16)),
        ],
        compiler_params=pltpu.CompilerParams(
            collective_id=0, has_side_effects=True, vmem_limit_bytes=VMEM_MIB * 1024 * 1024
        ),
    )(coarse_ids.T, a_tiles, prolong.reshape(2 * NB, T, T))


def solution(mesh):
    torus = Mesh(mesh.devices.reshape(4, 2, 2, 4, 4), GRP_DEV)

    def run(a_tiles, prolong, coarse_ids):
        return jax.shard_map(
            local,
            mesh=torus,
            in_specs=(P(GRP_DEV, None, None, None), P(GRP_DEV, None, None, None), P(GRP_DEV, None)),
            out_specs=P(GRP_DEV, None),
            check_vma=False,
        )(a_tiles, prolong, coarse_ids)

    return run
```

```python
import jax
import jax.numpy as jnp
from jax import lax
from jax.experimental import pallas as pl
from jax.experimental.pallas import tpu as pltpu
from jax.sharding import Mesh
from jax.sharding import PartitionSpec as P

GRP_DEV = ("grp_0", "grp_1", "grp_2", "dev_0", "dev_1")
AXES = GRP_DEV
NB = 32
T = 128
CT = 4
PZ = 192
VMEM_MIB = 53
F32 = jnp.float32
BF16 = jnp.bfloat16


def coords(index):
    grp, dev = index // 16, index % 16
    return (grp // 4, grp // 2 % 2, grp % 2, dev // 4, dev % 4)


def split(x):
    hi = x.astype(BF16)
    lo = (x - hi.astype(F32)).astype(BF16)
    return hi, lo


def rest(x):
    return x - x.astype(BF16).astype(F32)


def twice(x):
    return jnp.concatenate([x, x], axis=1)


def kernel(
    ids,
    a_hbm,
    p_hbm,
    out,
    a_buf,
    p_buf,
    pt,
    prod,
    r_even,
    r_odd,
    halo,
    halo_id,
    id_send,
    c_send,
    y_a,
    y_b,
    y_d,
    z_send,
    z_recv,
    e_send,
    e_y,
    e_pass,
    e_recv,
    t_send,
    t_one,
    t_two,
    sem_a,
    sem_p,
    sem_hs,
    sem_hr,
    sem_ys,
    sem_yr,
    sem_zs,
    sem_zr,
    sem_es,
    sem_er,
    sem_ts,
    sem_tr,
):
    gx, gz, gc, dz, dy = (lax.axis_index(name) for name in AXES)
    grp = gx * 4 + gz * 2 + gc
    dev = dz * 4 + dy
    me = grp * 16 + dev

    def dev_peer(rel):
        other = lax.rem(dev + rel, 16)
        return (gx, gz, gc, other // 4, lax.rem(other, 4))

    def grp_peer(rel):
        other = lax.rem(grp + rel, 16)
        return (other // 4, lax.rem(other // 2, 2), lax.rem(other, 2), dz, dy)

    def y_peer(rel):
        return (gx, gz, gc, dz, lax.rem(dy + rel, 4))

    def z_peer(rel):
        return (gx, gz, gc, lax.rem(dz + rel, 4), dy)

    def ring_peer(rel):
        other = lax.rem(me + rel, 256)
        g, d = other // 16, lax.rem(other, 16)
        return (g // 4, lax.rem(g // 2, 2), lax.rem(g, 2), d // 4, lax.rem(d, 4))

    def remote(src, dst, send, recv, peer):
        return pltpu.make_async_remote_copy(
            src_ref=src,
            dst_ref=dst,
            send_sem=send,
            recv_sem=recv,
            device_id=peer,
            device_id_type=pl.DeviceIdType.MESH,
        )

    def load_a(g):
        cut = pl.ds(g * 4, 4)
        return pltpu.make_async_copy(a_hbm.at[cut], a_buf.at[cut], sem_a.at[g])

    def load_p(g):
        cut = pl.ds(g * 8, 8)
        return pltpu.make_async_copy(p_hbm.at[cut], p_buf.at[cut], sem_p.at[g])

    load_p(0).start()
    load_a(0).start()
    load_a(1).start()
    load_p(7).start()
    for g in range(1, 7):
        load_p(g).start()
        load_a(g + 1).start()

    nxt, prv = ring_peer(1), ring_peer(255)
    barrier = pltpu.get_barrier_semaphore()
    with jax.named_scope("signals"):
        for peer in [nxt, prv] + [dev_peer(k) for k in range(1, 16)] + [grp_peer(k) for k in range(1, 16)]:
            pl.semaphore_signal(barrier, inc=1, device_id=peer, device_id_type=pl.DeviceIdType.MESH)

    zero_f = jnp.zeros((T, T), F32)
    zero_b = jnp.zeros((T, T), BF16)
    prod[PZ] = zero_f
    p_buf[64] = zero_f
    pt[64] = zero_b
    pt[129] = zero_b
    for side, block in ((0, 0), (1, NB - 1)):
        for slot in range(2):
            id_send[side, :, slot * T : (slot + 1) * T] = jnp.full((8, T), ids[slot, block], jnp.int32)

    def pick(block, j, first, none):
        return jnp.where(ids[0, block] == j, first, jnp.where(ids[1, block] == j, first + 1, none))

    def push_p(p0, p1, unit):
        h0, l0 = split(p0)
        h1, l1 = split(p1)
        high, low = jnp.concatenate([h0, h1], axis=1), jnp.concatenate([l0, l1], axis=1)
        pltpu.matmul_push_rhs(jnp.concatenate([high, low], axis=0), 0, unit)
        return (h0, h1), (l0, l1)

    def gather(n0, n1, n2, j, ends):
        total = prod[pick(n1, j, n1 * 6 + 2, PZ)]
        if ends != 0:
            total = total + prod[pick(n0, j, n0 * 6, PZ)]
        if ends != 1:
            total = total + prod[pick(n2, j, n2 * 6 + 4, PZ)]
        return total

    def r_at(pair, parity):
        return (r_even, r_odd)[parity].at[pair // 2]

    def put_r(pair, parity, half, j, value, block):
        into = r_at(pair, parity)
        into[0, j, half * T : (half + 1) * T] = value
        into[1, j, half * T : (half + 1) * T] = rest(value)
        both = value * p_buf[pick(block, j, block * 2, 64)]
        return jnp.sum(both.reshape(16, 8, T), axis=0)

    def assemble(pair, parity):
        total = jnp.zeros((8, T), F32)
        for half in range(2):
            block = pair * 2 - 1 + half
            for j in range(CT):
                value = gather(block - 1, block, block + 1, j, None)
                total = total + put_r(pair, parity, half, j, value, block)
        return total

    def body(acc, odd, tot):

        def products(t, into):
            for unit in range(2):
                n = t * 2 + unit
                high, low = push_p(p_buf[n * 2], p_buf[n * 2 + 1], unit)
                for slot in range(2):
                    pt[n * 2 + slot] = high[slot].T
                    pt[65 + n * 2 + slot] = low[slot].T
                for m in range(3):
                    tile = a_buf[jnp.clip(n + 1 - m, 0, NB - 1), m]
                    pltpu.matmul_acc_lhs(into[unit][m], twice(tile), load_staged_rhs=0 if m == 0 else None)
                    pltpu.matmul_acc_lhs(into[unit][m], twice(rest(tile)))

        def drain(t, into):
            for unit in range(2):
                n = t * 2 + unit
                for m in range(3):
                    res = pltpu.matmul_pop(into[unit][m])
                    prod[(n * 3 + m) * 2] = res[:, :T]
                    prod[(n * 3 + m) * 2 + 1] = res[:, T:]

        def one_group(g):
            products(g * 2, acc)
            products(g * 2 + 1, odd)
            drain(g * 2, acc)
            drain(g * 2 + 1, odd)

        def two_groups(k, carry):
            for u in (1, 2):
                load_p(k * 2 + u).wait()
                load_a(k * 2 + u + 1).wait()
            t = k * 4 + 2
            products(t, acc)
            products(t + 1, odd)
            drain(t, acc)
            products(t + 2, acc)
            drain(t + 1, odd)
            products(t + 3, odd)
            drain(t + 2, acc)
            drain(t + 3, odd)
            return carry

        with jax.named_scope("load"):
            load_p(0).wait()
            load_a(0).wait()
            load_a(1).wait()
        with jax.named_scope("right_start"):
            one_group(0)
        with jax.named_scope("right_loop"):
            lax.fori_loop(0, 2, two_groups, 0)
        load_p(7).wait()
        with jax.named_scope("barrier"):
            pl.semaphore_wait(barrier, 32)
        halo_copies = [
            remote(p_buf.at[pl.ds(62, 2)], halo.at[0], sem_hs.at[0], sem_hr.at[0], nxt),
            remote(p_buf.at[pl.ds(0, 2)], halo.at[1], sem_hs.at[1], sem_hr.at[1], prv),
            remote(id_send.at[1], halo_id.at[0], sem_hs.at[2], sem_hr.at[2], nxt),
            remote(id_send.at[0], halo_id.at[1], sem_hs.at[3], sem_hr.at[3], prv),
        ]
        for copy in halo_copies:
            copy.start()
        with jax.named_scope("right_loop"):
            lax.fori_loop(2, 3, two_groups, 0)
        with jax.named_scope("right_end"):
            one_group(7)

        ends = ((0, 0), (1, 15))

        def lhs(b0, b1, i, low):
            base = 65 if low else 0
            none = 129 if low else 64
            return jnp.concatenate(
                [pt[pick(b0, i, base + b0 * 2, none)], pt[pick(b1, i, base + b1 * 2, none)]], axis=1
            )

        def pair_step(chunk, pair, parity, b0, b1):
            read = r_at(pair, parity)

            def right(part):
                return jnp.concatenate([read[part, chunk * 2], read[part, chunk * 2 + 1]], axis=1)

            for unit in range(2):
                rows = (unit * 2, unit * 2 + 1)
                high = jnp.concatenate([lhs(b0, b1, i, False) for i in rows], axis=0)
                low = jnp.concatenate([lhs(b0, b1, i, True) for i in rows], axis=0)
                pltpu.matmul_push_rhs(right(0), 0, unit)
                pltpu.matmul_push_rhs(right(1), 1, unit)
                pltpu.matmul_acc_lhs(tot[unit], high, load_staged_rhs=0)
                pltpu.matmul_acc_lhs(tot[unit], low)
                pltpu.matmul_acc_lhs(tot[unit], high, load_staged_rhs=1)

        def finish(chunk):
            for unit in range(2):
                res = pltpu.matmul_pop(tot[unit])
                for half in range(2):
                    i = unit * 2 + half
                    for y in range(4):
                        c_send[chunk, y, i] = res[half * T + y * 32 : half * T + (y + 1) * 32]

        def four_first(k, total):
            for u in range(4):
                pair = k * 4 + 1 + u
                pair_step(0, pair, (1 + u) % 2, pair * 2 - 1, pair * 2)
                total = total + assemble(pair + 1, u % 2)
            return total

        def four_second(k, carry):
            for u in range(4):
                pair = k * 4 + 1 + u
                pair_step(1, pair, (1 + u) % 2, pair * 2 - 1, pair * 2)
            return carry

        with jax.named_scope("assemble"):
            total = assemble(1, 1)
        with jax.named_scope("left_loop_0"):
            total = lax.fori_loop(0, 3, four_first, total)
        with jax.named_scope("left_end_0"):
            pair_step(0, 13, 1, 25, 26)
            total = total + assemble(14, 0)
            pair_step(0, 14, 0, 27, 28)
            total = total + assemble(15, 1)
            pair_step(0, 15, 1, 29, 30)

        with jax.named_scope("halo_wait"):
            for copy in halo_copies:
                copy.wait_recv()
        for side in range(2):
            push_p(halo[side, 0], halo[side, 1], side)
            tile = a_buf[0, 0] if side == 0 else a_buf[NB - 1, 2]
            pltpu.matmul_acc_lhs(acc[side][0], twice(tile), load_staged_rhs=0)
            pltpu.matmul_acc_lhs(acc[side][0], twice(rest(tile)))
        edge = [pltpu.matmul_pop(acc[side][0]) for side in range(2)]
        for side in range(2):
            prod[193 + side * 2] = edge[side][:, :T]
            prod[194 + side * 2] = edge[side][:, T:]
        inner = [dev > 0, dev < 15]
        for half, side in ((0, 1), (1, 0)):
            for j in range(CT):
                own = gather(30, 31, 31, j, 1) if side == 1 else gather(0, 0, 1, j, 0)
                extra = zero_f
                for slot in range(2):
                    match = halo_id[side, 0:1, slot * T : (slot + 1) * T] == j
                    extra = extra + jnp.where(match, prod[193 + side * 2 + slot], 0.0)
                block = 0 if half == 1 else NB - 1
                total = total + put_r(0, 0, half, j, own + jnp.where(inner[side], extra, 0.0), block)

        pair_step(0, 0, 0, NB - 1, 0)
        finish(0)


        def edge_y(side, rel):
            other = lax.rem(dy + rel, 4)
            return remote(
                e_send.at[side, other], e_y.at[side], sem_es.at[side, rel - 1], sem_er.at[side, 0], y_peer(rel)
            )

        def edge_z(side, rel):
            other = lax.rem(dz + rel, 4)
            return remote(
                e_pass.at[side, other], e_recv.at[side], sem_es.at[side, rel + 2], sem_er.at[side, 1], z_peer(rel)
            )

        def start_edges():
            for side, at in ends:

                @pl.when(dev == at)
                def _(side=side, at=at):
                    block = 0 if side == 0 else NB - 1
                    y0, y1 = prod[193 + side * 2], prod[194 + side * 2]
                    wide = jnp.concatenate([y0, y1], axis=1)
                    for part in (wide, rest(wide)):
                        for unit in range(2):
                            pltpu.matmul_push_rhs(jnp.concatenate([part, part], axis=0), 0, unit)
                            left = jnp.concatenate([pt[block * 2 + unit], pt[65 + block * 2 + unit]], axis=1)
                            pltpu.matmul_acc_lhs(acc[unit][0], left, load_staged_rhs=0)
                    for unit in range(2):
                        res = pltpu.matmul_pop(acc[unit][0])
                        for y in range(4):
                            e_send[side, y, unit * 32 : (unit + 1) * 32] = res[y * 32 : (y + 1) * 32]
                    upper = lax.broadcasted_iota(jnp.int32, (8, 2 * T), 0) < 4
                    code = jnp.where(upper, halo_id[side], id_send[side]).astype(F32)
                    for y in range(4):
                        e_send[side, y, 64:72] = code
                    for rel in range(1, 4):
                        edge_y(side, rel).start()
                    e_y[side] = e_send[side, at % 4]

        def pass_edges():
            for side, at in ends:

                @pl.when(dz == at // 4)
                def _(side=side, at=at):
                    @pl.when(dy != at % 4)
                    def _():
                        edge_y(side, 1).wait_recv()

                    for z in range(4):
                        for part in range(2):
                            half = slice(part * T, (part + 1) * T)
                            value = jnp.zeros((32, T), F32)
                            for slot in range(2):
                                match = e_y[side, 68:69, slot * T : (slot + 1) * T] == float(z)
                                value = value + jnp.where(match, e_y[side, slot * 32 : (slot + 1) * 32, half], 0.0)
                            e_pass[side, z, 0:32, half] = value
                        e_pass[side, z, 32:40] = e_y[side, 64:72]
                    for rel in range(1, 4):
                        edge_z(side, rel).start()
                    e_recv[side] = e_pass[side, at // 4]

        up, down = lax.rem(dy + 1, 4), lax.rem(dy + 3, 4)
        far = lax.rem(dy + 2, 4)
        lo2, hi2 = pl.ds(0, 2), pl.ds(2, 2)

        def y_first(c):
            return [
                remote(c_send.at[c, far, lo2], y_a.at[c, 0], sem_ys.at[c, 0], sem_yr.at[c, 0], y_peer(1)),
                remote(c_send.at[c, far, hi2], y_a.at[c, 1], sem_ys.at[c, 1], sem_yr.at[c, 1], y_peer(3)),
                remote(c_send.at[c, up, hi2], y_d.at[c, 0], sem_ys.at[c, 2], sem_yr.at[c, 2], y_peer(1)),
                remote(c_send.at[c, down, lo2], y_d.at[c, 1], sem_ys.at[c, 3], sem_yr.at[c, 3], y_peer(3)),
            ]

        def y_second(c):
            return [
                remote(c_send.at[c, up, lo2], y_b.at[c, 0], sem_ys.at[c, 4], sem_yr.at[c, 4], y_peer(1)),
                remote(c_send.at[c, down, hi2], y_b.at[c, 1], sem_ys.at[c, 5], sem_yr.at[c, 5], y_peer(3)),
            ]

        def z_all(c):
            return [
                remote(
                    z_send.at[c, lax.rem(dz + rel, 4)],
                    z_recv.at[c, rel - 1],
                    sem_zs.at[c, rel - 1],
                    sem_zr.at[c, rel - 1],
                    z_peer(rel),
                )
                for rel in range(1, 4)
            ]

        def begin_second(c):
            first = y_first(c)
            first[0].wait_recv()
            c_send[c, up, lo2] = c_send[c, up, lo2] + y_a[c, 0]
            y_second(c)[0].start()
            first[1].wait_recv()
            c_send[c, down, hi2] = c_send[c, down, hi2] + y_a[c, 1]
            y_second(c)[1].start()

        def begin_z(c):
            for copy in y_first(c)[2:] + y_second(c):
                copy.wait_recv()
            z_send[c, 0:2] = c_send[c, dy, lo2] + y_b[c, 0] + y_d[c, 1]
            z_send[c, 2:4] = c_send[c, dy, hi2] + y_b[c, 1] + y_d[c, 0]
            for copy in z_all(c):
                copy.start()

        def t_copies(phase):
            into = t_one if phase == 0 else t_two
            row = pl.ds(0, 1)
            peer = dev_peer if phase == 0 else grp_peer
            return [
                remote(t_send.at[phase, row], into.at[rel, row], sem_ts.at[phase, rel], sem_tr.at[phase, rel], peer(rel))
                for rel in range(1, 16)
            ]

        one, two = t_copies(0), t_copies(1)

        def start(copies):
            for copy in copies:
                copy.start()

        total = jnp.sum(total, axis=0, keepdims=True)
        t_send[0, 0:1] = total
        start(one)
        start(y_first(0)[:2])
        with jax.named_scope("edges"):
            start_edges()
        with jax.named_scope("left_loop_1"):
            lax.fori_loop(0, 1, four_second, 0)
        start(y_first(0)[2:])
        with jax.named_scope("left_loop_1"):
            lax.fori_loop(1, 3, four_second, 0)
        for pair in (13, 14, 15):
            pair_step(1, pair, pair % 2, pair * 2 - 1, pair * 2)
        pair_step(1, 0, 0, NB - 1, 0)
        finish(1)
        start(y_first(1)[:2])
        with jax.named_scope("y_second_0"):
            begin_second(0)
        start(y_first(1)[2:])
        with jax.named_scope("trace_dev"):
            for rel in range(1, 16):
                one[rel - 1].wait_recv()
                total = total + t_one[rel, 0:1]
            t_send[1, 0:1] = total
            start(two)
        with jax.named_scope("y_second_1"):
            begin_second(1)
        with jax.named_scope("edge_pass"):
            pass_edges()
        with jax.named_scope("z_0"):
            begin_z(0)
        with jax.named_scope("z_1"):
            begin_z(1)
        with jax.named_scope("trace_grp"):
            for rel in range(1, 16):
                two[rel - 1].wait_recv()
                total = total + t_two[rel, 0:1]
        mean = jnp.sum(total, axis=(0, 1), keepdims=True) * (1.0 / 8192.0)
        scale = jnp.broadcast_to(mean, (32, 2 * T))

        for side, at in ends:
            base = 0 if side == 0 else 1024

            with jax.named_scope("edge_wait"):

                @pl.when(dz != at // 4)
                def _(side=side):
                    edge_z(side, 1).wait_recv()

            for j in range(CT):
                value = jnp.zeros((32, T), F32)
                for slot in range(2):
                    match = e_recv[side, 32:33, slot * T : (slot + 1) * T] == float(j)
                    value = value + jnp.where(match, e_recv[side, 0:32, slot * T : (slot + 1) * T], 0.0)
                out[:, base + j * T : base + (j + 1) * T] = value / scale[:, :T]

        for c in range(2):
            value = z_send[c, dz]
            with jax.named_scope("z_wait"):
                for k, copy in enumerate(z_all(c)):
                    copy.wait_recv()
                    value = value + z_recv[c, k]
            out[:, 512 + c * 256 : 512 + (c + 1) * 256] = value / scale

        done = jax.named_scope("sends_done")
        done.__enter__()
        for copy in halo_copies + one + two:
            copy.wait_send()
        for c in range(2):
            for copy in y_first(c) + y_second(c) + z_all(c):
                copy.wait_send()
        for side, at in ends:

            @pl.when(dev == at)
            def _(side=side):
                for rel in range(1, 4):
                    edge_y(side, rel).wait_send()

            @pl.when(dz == at // 4)
            def _(side=side):
                for rel in range(1, 4):
                    edge_z(side, rel).wait_send()

        done.__exit__(None, None, None)

    small, other = (
        tuple(tuple(pltpu.ACC(unit)((T, 2 * T), F32) for _ in range(3)) for unit in range(2)) for _ in range(2)
    )
    large = tuple(pltpu.ACC(unit)((2 * T, 2 * T), F32) for unit in range(2))
    pl.run_scoped(body, small, other, large)


def local(a_tiles, prolong, coarse_ids):
    vmem, dma = pltpu.VMEM, pltpu.SemaphoreType.DMA
    return pl.pallas_call(
        kernel,
        out_shape=jax.ShapeDtypeStruct((32, 1536), F32),
        in_specs=[
            pl.BlockSpec(memory_space=pltpu.SMEM),
            pl.BlockSpec(memory_space=pltpu.HBM),
            pl.BlockSpec(memory_space=pltpu.HBM),
        ],
        out_specs=pl.BlockSpec(memory_space=pltpu.VMEM),
        scratch_shapes=[
            vmem((NB, 3, T, T), F32),
            vmem((65, T, T), F32),
            vmem((130, T, T), BF16),
            vmem((197, T, T), F32),
            vmem((8, 2, 4, 2 * T, T), F32),
            vmem((8, 2, 4, 2 * T, T), F32),
            vmem((2, 2, T, T), F32),
            vmem((2, 8, 2 * T), jnp.int32),
            vmem((2, 8, 2 * T), jnp.int32),
            vmem((2, 4, 4, 32, 2 * T), F32),
            vmem((2, 2, 2, 32, 2 * T), F32),
            vmem((2, 2, 2, 32, 2 * T), F32),
            vmem((2, 2, 2, 32, 2 * T), F32),
            vmem((2, 4, 32, 2 * T), F32),
            vmem((2, 3, 32, 2 * T), F32),
            vmem((2, 4, 72, 2 * T), F32),
            vmem((2, 72, 2 * T), F32),
            vmem((2, 4, 40, 2 * T), F32),
            vmem((2, 40, 2 * T), F32),
            vmem((2, 8, T), F32),
            vmem((16, 8, T), F32),
            vmem((16, 8, T), F32),
            dma((8,)),
            dma((8,)),
            dma((4,)),
            dma((4,)),
            dma((2, 6)),
            dma((2, 6)),
            dma((2, 6)),
            dma((2, 6)),
            dma((2, 6)),
            dma((2, 2)),
            dma((2, 16)),
            dma((2, 16)),
        ],
        compiler_params=pltpu.CompilerParams(
            collective_id=0, has_side_effects=True, vmem_limit_bytes=VMEM_MIB * 1024 * 1024
        ),
    )(coarse_ids.T, a_tiles, prolong.reshape(2 * NB, T, T))


def solution(mesh):
    torus = Mesh(mesh.devices.reshape(4, 2, 2, 4, 4), GRP_DEV)

    def run(a_tiles, prolong, coarse_ids):
        return jax.shard_map(
            local,
            mesh=torus,
            in_specs=(P(GRP_DEV, None, None, None), P(GRP_DEV, None, None, None), P(GRP_DEV, None)),
            out_specs=P(GRP_DEV, None),
            check_vma=False,
        )(a_tiles, prolong, coarse_ids)

    return run
```

```python
import jax
import jax.numpy as jnp
from jax import lax
from jax.experimental import pallas as pl
from jax.experimental.pallas import tpu as pltpu
from jax.sharding import Mesh
from jax.sharding import PartitionSpec as P

GRP_DEV = ("grp_0", "grp_1", "grp_2", "dev_0", "dev_1")
AXES = GRP_DEV
NB = 32
T = 128
CT = 4
PZ = 192
OFFSETS = (2, 1, 3, 0)
VMEM_MIB = 53
F32 = jnp.float32
BF16 = jnp.bfloat16


def coords(index):
    grp, dev = index // 16, index % 16
    return (grp // 4, grp // 2 % 2, grp % 2, dev // 4, dev % 4)


def split(x):
    hi = x.astype(BF16)
    lo = (x - hi.astype(F32)).astype(BF16)
    return hi, lo


def rest(x):
    return x - x.astype(BF16).astype(F32)


def twice(x):
    return jnp.concatenate([x, x], axis=1)


def kernel(
    ids,
    a_hbm,
    p_hbm,
    out,
    a_buf,
    p_buf,
    pt,
    prod,
    r_even,
    r_odd,
    halo,
    halo_id,
    id_send,
    c_send,
    y_recv,
    z_send,
    z_recv,
    e_send,
    e_y,
    e_pass,
    e_recv,
    t_send,
    t_recv,
    sem_a,
    sem_p,
    sem_hs,
    sem_hr,
    sem_ys,
    sem_yr,
    sem_zs,
    sem_zr,
    sem_es,
    sem_er,
    sem_ts,
    sem_tr,
):
    gx, gz, gc, dz, dy = (lax.axis_index(name) for name in AXES)
    grp = gx * 4 + gz * 2 + gc
    dev = dz * 4 + dy
    me = grp * 16 + dev

    def dev_peer(rel):
        other = lax.rem(dev + rel, 16)
        return (gx, gz, gc, other // 4, lax.rem(other, 4))

    def grp_peer(rel):
        other = lax.rem(grp + rel, 16)
        return (other // 4, lax.rem(other // 2, 2), lax.rem(other, 2), dz, dy)

    def y_peer(rel):
        return (gx, gz, gc, dz, lax.rem(dy + rel, 4))

    def z_peer(rel):
        return (gx, gz, gc, lax.rem(dz + rel, 4), dy)

    def ring_peer(rel):
        other = lax.rem(me + rel, 256)
        g, d = other // 16, lax.rem(other, 16)
        return (g // 4, lax.rem(g // 2, 2), lax.rem(g, 2), d // 4, lax.rem(d, 4))

    def remote(src, dst, send, recv, peer):
        return pltpu.make_async_remote_copy(
            src_ref=src,
            dst_ref=dst,
            send_sem=send,
            recv_sem=recv,
            device_id=peer,
            device_id_type=pl.DeviceIdType.MESH,
        )

    def load_a(g):
        cut = pl.ds(g * 4, 4)
        return pltpu.make_async_copy(a_hbm.at[cut], a_buf.at[cut], sem_a.at[g])

    def load_p(g):
        cut = pl.ds(g * 8, 8)
        return pltpu.make_async_copy(p_hbm.at[cut], p_buf.at[cut], sem_p.at[g])

    load_p(0).start()
    load_a(0).start()
    load_a(1).start()
    load_p(7).start()
    for g in range(1, 7):
        load_p(g).start()
        load_a(g + 1).start()

    nxt, prv = ring_peer(1), ring_peer(255)
    barrier = pltpu.get_barrier_semaphore()
    peers = [nxt, prv] + [dev_peer(k) for k in range(1, 16)] + [grp_peer(k) for k in range(1, 16)]
    with jax.named_scope("signals"):
        for peer in peers:
            pl.semaphore_signal(barrier, inc=1, device_id=peer, device_id_type=pl.DeviceIdType.MESH)

    zero_f = jnp.zeros((T, T), F32)
    zero_b = jnp.zeros((T, T), BF16)
    prod[PZ] = zero_f
    p_buf[64] = zero_f
    pt[64] = zero_b
    pt[129] = zero_b
    for side, block in ((0, 0), (1, NB - 1)):
        for slot in range(2):
            id_send[side, :, slot * T : (slot + 1) * T] = jnp.full((8, T), ids[slot, block], jnp.int32)

    def pick(block, j, first, none):
        return jnp.where(ids[0, block] == j, first, jnp.where(ids[1, block] == j, first + 1, none))

    def push_p(p0, p1, unit):
        h0, l0 = split(p0)
        h1, l1 = split(p1)
        high, low = jnp.concatenate([h0, h1], axis=1), jnp.concatenate([l0, l1], axis=1)
        pltpu.matmul_push_rhs(jnp.concatenate([high, low], axis=0), 0, unit)
        return (h0, h1), (l0, l1)

    def r_at(pair, parity):
        return (r_even, r_odd)[parity].at[pair // 2]

    def put_r(pair, parity, half, j, terms, block, extra=None):
        into = r_at(pair, parity)
        own = pick(block, j, block * 2, 64)
        total = jnp.zeros((8, T), F32)
        for k in range(4):
            rows = pl.ds(k * 32, 32)
            value = prod[terms[0], rows] + prod[terms[1], rows]
            if len(terms) == 3:
                value = value + prod[terms[2], rows]
            if extra is not None:
                value = value + extra[k * 32 : (k + 1) * 32]
            place = pl.ds(half * T + k * 32, 32)
            into[0, j, place] = value
            into[1, j, place] = rest(value)
            total = total + jnp.sum((value * p_buf[own, rows]).reshape(4, 8, T), axis=0)
        return total

    def assemble(pair, parity):
        total = jnp.zeros((8, T), F32)
        for half in range(2):
            block = pair * 2 - 1 + half
            for j in range(CT):
                terms = [pick(block - 1 + m, j, (block - 1 + m) * 6 + m * 2, PZ) for m in range(3)]
                total = total + put_r(pair, parity, half, j, terms, block)
        return total

    def body(acc, odd):

        def products(t, into):
            for unit in range(2):
                n = t * 2 + unit
                high, low = push_p(p_buf[n * 2], p_buf[n * 2 + 1], unit)
                for slot in range(2):
                    pt[n * 2 + slot] = high[slot].T
                    pt[65 + n * 2 + slot] = low[slot].T
                for m in range(3):
                    tile = a_buf[jnp.clip(n + 1 - m, 0, NB - 1), m]
                    pltpu.matmul_acc_lhs(into[unit][m], twice(tile), load_staged_rhs=0 if m == 0 else None)
                    pltpu.matmul_acc_lhs(into[unit][m], twice(rest(tile)))

        def drain(t, into):
            for unit in range(2):
                n = t * 2 + unit
                for m in range(3):
                    res = pltpu.matmul_pop(into[unit][m])
                    prod[(n * 3 + m) * 2] = res[:, :T]
                    prod[(n * 3 + m) * 2 + 1] = res[:, T:]

        def one_group(g):
            products(g * 2, acc)
            products(g * 2 + 1, odd)
            drain(g * 2, acc)
            drain(g * 2 + 1, odd)

        def two_groups(k, carry):
            for u in (1, 2):
                load_p(k * 2 + u).wait()
                load_a(k * 2 + u + 1).wait()
            t = k * 4 + 2
            products(t, acc)
            products(t + 1, odd)
            drain(t, acc)
            products(t + 2, acc)
            drain(t + 1, odd)
            products(t + 3, odd)
            drain(t + 2, acc)
            drain(t + 3, odd)
            return carry

        with jax.named_scope("load"):
            load_p(0).wait()
            load_a(0).wait()
            load_a(1).wait()
        with jax.named_scope("right_start"):
            one_group(0)
        with jax.named_scope("right_loop"):
            lax.fori_loop(0, 1, two_groups, 0)
        load_p(7).wait()
        with jax.named_scope("barrier"):
            pl.semaphore_wait(barrier, 32)
        halo_copies = [
            remote(p_buf.at[pl.ds(62, 2)], halo.at[0], sem_hs.at[0], sem_hr.at[0], nxt),
            remote(p_buf.at[pl.ds(0, 2)], halo.at[1], sem_hs.at[1], sem_hr.at[1], prv),
            remote(id_send.at[1], halo_id.at[0], sem_hs.at[2], sem_hr.at[2], nxt),
            remote(id_send.at[0], halo_id.at[1], sem_hs.at[3], sem_hr.at[3], prv),
        ]
        for copy in halo_copies:
            copy.start()
        with jax.named_scope("right_loop"):
            lax.fori_loop(1, 3, two_groups, 0)
        with jax.named_scope("right_end"):
            one_group(7)

        ends = ((0, 0), (1, 15))

        def lhs(b0, b1, i, low):
            base = 65 if low else 0
            none = 129 if low else 64
            return jnp.concatenate(
                [pt[pick(b0, i, base + b0 * 2, none)], pt[pick(b1, i, base + b1 * 2, none)]], axis=1
            )

        def pair_step(part, pair, parity, b0, b1):
            read = r_at(pair, parity)
            tiles = [lax.rem(dz + OFFSETS[part * 2 + t], 4) for t in range(2)]
            high, low = ([lhs(b0, b1, i, under) for i in tiles] for under in (False, True))
            into = (odd, acc)[part]

            def push(level):
                for unit in range(2):
                    right = jnp.concatenate([read[level, unit * 2], read[level, unit * 2 + 1]], axis=1)
                    pltpu.matmul_push_rhs(right, level, unit)

            push(0)
            for left, t, staged in ((low, 0, 0), (high, 0, None), (low, 1, None), (high, 1, None)):
                for unit in range(2):
                    pltpu.matmul_acc_lhs(into[unit][t], left[t], load_staged_rhs=staged)
            push(1)
            for left, t, staged in ((high, 1, 1), (high, 0, None)):
                for unit in range(2):
                    pltpu.matmul_acc_lhs(into[unit][t], left[t], load_staged_rhs=staged)

        def finish(part):
            for t in range(2):
                for unit in range(2):
                    res = pltpu.matmul_pop((odd, acc)[part][unit][t])
                    for y in range(4):
                        c_send[part * 2 + t, y, :, unit * 2 * T : (unit + 1) * 2 * T] = res[y * 32 : (y + 1) * 32]

        def four_first(k, total):
            for u in range(4):
                pair = k * 4 + 1 + u
                pair_step(0, pair, (1 + u) % 2, pair * 2 - 1, pair * 2)
                total = total + assemble(pair + 1, u % 2)
            return total

        def four_second(k, carry):
            for u in range(4):
                pair = lax.rem(k * 4 + 1 + u, 16)
                pair_step(1, pair, (1 + u) % 2, lax.rem(pair * 2 + 31, 32), pair * 2)
            return carry

        with jax.named_scope("assemble"):
            total = assemble(1, 1)
        with jax.named_scope("left_loop_0"):
            total = lax.fori_loop(0, 3, four_first, total)
        with jax.named_scope("left_end_0"):
            pair_step(0, 13, 1, 25, 26)
            total = total + assemble(14, 0)
            pair_step(0, 14, 0, 27, 28)
            total = total + assemble(15, 1)
            pair_step(0, 15, 1, 29, 30)

        with jax.named_scope("halo_wait"):
            for copy in halo_copies:
                copy.wait_recv()
        for side in range(2):
            push_p(halo[side, 0], halo[side, 1], side)
            tile = a_buf[0, 0] if side == 0 else a_buf[NB - 1, 2]
            pltpu.matmul_acc_lhs(acc[side][0], twice(tile), load_staged_rhs=0)
            pltpu.matmul_acc_lhs(acc[side][0], twice(rest(tile)))
        edge = [pltpu.matmul_pop(acc[side][0]) for side in range(2)]
        for side in range(2):
            prod[193 + side * 2] = edge[side][:, :T]
            prod[194 + side * 2] = edge[side][:, T:]
        inner = [dev > 0, dev < 15]
        for half, side in ((0, 1), (1, 0)):
            for j in range(CT):
                block = 0 if half == 1 else NB - 1
                terms = [pick(block, j, block * 6 + 2, PZ)]
                terms += [pick(30, j, 180, PZ)] if side == 1 else [pick(1, j, 10, PZ)]
                extra = zero_f
                for slot in range(2):
                    match = halo_id[side, 0:1, slot * T : (slot + 1) * T] == j
                    extra = extra + jnp.where(match, prod[193 + side * 2 + slot], 0.0)
                total = total + put_r(0, 0, half, j, terms, block, jnp.where(inner[side], extra, 0.0))

        def edge_y(side, rel):
            other = lax.rem(dy + rel, 4)
            return remote(
                e_send.at[side, other], e_y.at[side], sem_es.at[side, rel - 1], sem_er.at[side, 0], y_peer(rel)
            )

        def edge_z(side, rel):
            other = lax.rem(dz + rel, 4)
            return remote(
                e_pass.at[side, other], e_recv.at[side], sem_es.at[side, rel + 2], sem_er.at[side, 1], z_peer(rel)
            )

        def start_edges():
            for side, at in ends:

                @pl.when(dev == at)
                def _(side=side, at=at):
                    block = 0 if side == 0 else NB - 1
                    y0, y1 = prod[193 + side * 2], prod[194 + side * 2]
                    wide = jnp.concatenate([y0, y1], axis=1)
                    for part in (wide, rest(wide)):
                        for unit in range(2):
                            pltpu.matmul_push_rhs(jnp.concatenate([part, part], axis=0), 0, unit)
                            left = jnp.concatenate([pt[block * 2 + unit], pt[65 + block * 2 + unit]], axis=1)
                            pltpu.matmul_acc_lhs(acc[unit][0], left, load_staged_rhs=0)
                    for unit in range(2):
                        res = pltpu.matmul_pop(acc[unit][0])
                        for y in range(4):
                            e_send[side, y, unit * 32 : (unit + 1) * 32] = res[y * 32 : (y + 1) * 32]
                    upper = lax.broadcasted_iota(jnp.int32, (8, 2 * T), 0) < 4
                    code = jnp.where(upper, halo_id[side], id_send[side]).astype(F32)
                    for y in range(4):
                        e_send[side, y, 64:72] = code
                    for rel in range(1, 4):
                        edge_y(side, rel).start()
                    e_y[side] = e_send[side, at % 4]

        def pass_edges():
            for side, at in ends:

                @pl.when(dz == at // 4)
                def _(side=side, at=at):
                    @pl.when(dy != at % 4)
                    def _():
                        edge_y(side, 1).wait_recv()

                    for z in range(4):
                        for part in range(2):
                            half = slice(part * T, (part + 1) * T)
                            value = jnp.zeros((32, T), F32)
                            for slot in range(2):
                                match = e_y[side, 68:69, slot * T : (slot + 1) * T] == float(z)
                                value = value + jnp.where(match, e_y[side, slot * 32 : (slot + 1) * 32, half], 0.0)
                            e_pass[side, z, 0:32, half] = value
                        e_pass[side, z, 32:40] = e_y[side, 64:72]
                    for rel in range(1, 4):
                        edge_z(side, rel).start()
                    e_recv[side] = e_pass[side, at // 4]

        def t_copies(phase):
            row = pl.ds(0, 1)
            peer = (dev_peer, grp_peer)[phase]
            return [
                remote(
                    t_send.at[phase, row],
                    t_recv.at[phase, rel, row],
                    sem_ts.at[phase, rel],
                    sem_tr.at[phase, rel],
                    peer(rel),
                )
                for rel in range(1, 16)
            ]

        def t_begin(phase, total):
            t_send[phase, 0:1] = total
            start(t_copies(phase))

        def t_sum(phase, total):
            for rel, copy in enumerate(t_copies(phase)):
                copy.wait_recv()
                total = total + t_recv[phase, rel + 1, 0:1]
            return total

        def start(copies):
            for copy in copies:
                copy.start()

        total = jnp.sum(total, axis=0, keepdims=True)
        t_begin(0, total)
        pair_step(0, 0, 0, NB - 1, 0)
        finish(0)

        def y_all(c):
            return [
                remote(
                    c_send.at[c, lax.rem(dy + rel, 4)],
                    y_recv.at[c, rel - 1],
                    sem_ys.at[c, rel - 1],
                    sem_yr.at[c, rel - 1],
                    y_peer(rel),
                )
                for rel in range(1, 4)
            ]

        def z_one(c):
            return remote(z_send.at[c], z_recv.at[c], sem_zs.at[c], sem_zr.at[c], z_peer(OFFSETS[c]))

        def y_sum(c):
            value = c_send[c, dy]
            for k, copy in enumerate(y_all(c)):
                copy.wait_recv()
                value = value + y_recv[c, k]
            return value

        def begin_z(c):
            z_send[c] = y_sum(c)
            z_one(c).start()

        start(y_all(0))
        with jax.named_scope("edges"):
            start_edges()
        start(y_all(1))
        with jax.named_scope("left_loop"):
            lax.fori_loop(0, 4, four_second, 0)
            finish(1)
        start(y_all(2))
        start(y_all(3))
        with jax.named_scope("z_0"):
            begin_z(0)
        with jax.named_scope("trace_dev"):
            total = t_sum(0, total)
            t_begin(1, total)
        with jax.named_scope("edge_pass"):
            pass_edges()
        with jax.named_scope("z_1"):
            begin_z(1)
        with jax.named_scope("z_2"):
            begin_z(2)
        with jax.named_scope("y_3"):
            mine = y_sum(3)
        with jax.named_scope("trace_grp"):
            total = t_sum(1, total)
        mean = jnp.sum(total, axis=(0, 1), keepdims=True) * (1.0 / 8192.0)
        scale = jnp.broadcast_to(mean, (32, 2 * T))

        for side, at in ends:
            base = 0 if side == 0 else 1024

            with jax.named_scope("edge_wait"):

                @pl.when(dz != at // 4)
                def _(side=side):
                    edge_z(side, 1).wait_recv()

            for j in range(CT):
                value = jnp.zeros((32, T), F32)
                for slot in range(2):
                    match = e_recv[side, 32:33, slot * T : (slot + 1) * T] == float(j)
                    value = value + jnp.where(match, e_recv[side, 0:32, slot * T : (slot + 1) * T], 0.0)
                out[:, base + j * T : base + (j + 1) * T] = value / scale[:, :T]

        with jax.named_scope("z_wait"):
            for c in range(3):
                z_one(c).wait_recv()
                mine = mine + z_recv[c]
        out[:, 512:1024] = mine / jnp.broadcast_to(mean, (32, 4 * T))

        done = jax.named_scope("sends_done")
        done.__enter__()
        for copy in halo_copies + t_copies(0) + t_copies(1):
            copy.wait_send()
        for c in range(4):
            for copy in y_all(c):
                copy.wait_send()
        for c in range(3):
            z_one(c).wait_send()
        for side, at in ends:

            @pl.when(dev == at)
            def _(side=side):
                for rel in range(1, 4):
                    edge_y(side, rel).wait_send()

            @pl.when(dz == at // 4)
            def _(side=side):
                for rel in range(1, 4):
                    edge_z(side, rel).wait_send()

        done.__exit__(None, None, None)

    small, other = (
        tuple(tuple(pltpu.ACC(unit)((T, 2 * T), F32) for _ in range(3)) for unit in range(2)) for _ in range(2)
    )
    pl.run_scoped(body, small, other)


def local(a_tiles, prolong, coarse_ids):
    vmem, dma = pltpu.VMEM, pltpu.SemaphoreType.DMA
    return pl.pallas_call(
        kernel,
        out_shape=jax.ShapeDtypeStruct((32, 1536), F32),
        in_specs=[
            pl.BlockSpec(memory_space=pltpu.SMEM),
            pl.BlockSpec(memory_space=pltpu.HBM),
            pl.BlockSpec(memory_space=pltpu.HBM),
        ],
        out_specs=pl.BlockSpec(memory_space=pltpu.VMEM),
        scratch_shapes=[
            vmem((NB, 3, T, T), F32),
            vmem((65, T, T), F32),
            vmem((130, T, T), BF16),
            vmem((197, T, T), F32),
            vmem((8, 2, 4, 2 * T, T), F32),
            vmem((8, 2, 4, 2 * T, T), F32),
            vmem((2, 2, T, T), F32),
            vmem((2, 8, 2 * T), jnp.int32),
            vmem((2, 8, 2 * T), jnp.int32),
            vmem((4, 4, 32, 4 * T), F32),
            vmem((4, 3, 32, 4 * T), F32),
            vmem((3, 32, 4 * T), F32),
            vmem((3, 32, 4 * T), F32),
            vmem((2, 4, 72, 2 * T), F32),
            vmem((2, 72, 2 * T), F32),
            vmem((2, 4, 40, 2 * T), F32),
            vmem((2, 40, 2 * T), F32),
            vmem((2, 8, T), F32),
            vmem((2, 16, 8, T), F32),
            dma((8,)),
            dma((8,)),
            dma((4,)),
            dma((4,)),
            dma((4, 3)),
            dma((4, 3)),
            dma((3,)),
            dma((3,)),
            dma((2, 6)),
            dma((2, 2)),
            dma((2, 16)),
            dma((2, 16)),
        ],
        compiler_params=pltpu.CompilerParams(
            collective_id=0, has_side_effects=True, vmem_limit_bytes=VMEM_MIB * 1024 * 1024
        ),
    )(coarse_ids.T, a_tiles, prolong.reshape(2 * NB, T, T))


def solution(mesh):
    torus = Mesh(mesh.devices.reshape(4, 2, 2, 4, 4), GRP_DEV)

    def run(a_tiles, prolong, coarse_ids):
        return jax.shard_map(
            local,
            mesh=torus,
            in_specs=(P(GRP_DEV, None, None, None), P(GRP_DEV, None, None, None), P(GRP_DEV, None)),
            out_specs=P(GRP_DEV, None),
            check_vma=False,
        )(a_tiles, prolong, coarse_ids)

    return run
```

```python
import jax
import jax.numpy as jnp
from jax import lax
from jax.experimental import pallas as pl
from jax.experimental.pallas import tpu as pltpu
from jax.sharding import Mesh
from jax.sharding import PartitionSpec as P

GRP_DEV = ("grp_0", "grp_1", "grp_2", "dev_0", "dev_1")
AXES = GRP_DEV
NB = 32
T = 128
CT = 4
PZ = 192
OFFSETS = (2, 1, 3, 0)
VMEM_MIB = 53
F32 = jnp.float32
BF16 = jnp.bfloat16


def coords(index):
    grp, dev = index // 16, index % 16
    return (grp // 4, grp // 2 % 2, grp % 2, dev // 4, dev % 4)


def split(x):
    hi = x.astype(BF16)
    lo = (x - hi.astype(F32)).astype(BF16)
    return hi, lo


def rest(x):
    return x - x.astype(BF16).astype(F32)


def twice(x):
    return jnp.concatenate([x, x], axis=1)


def kernel(
    ids,
    a_hbm,
    p_hbm,
    out,
    a_buf,
    p_buf,
    pt,
    prod,
    r_even,
    r_odd,
    halo,
    halo_id,
    id_send,
    c_send,
    y_recv,
    z_send,
    z_recv,
    e_send,
    e_y,
    e_pass,
    e_recv,
    t_send,
    t_recv,
    sem_a,
    sem_p,
    sem_hs,
    sem_hr,
    sem_ys,
    sem_yr,
    sem_zs,
    sem_zr,
    sem_es,
    sem_er,
    sem_ts,
    sem_tr,
):
    gx, gz, gc, dz, dy = (lax.axis_index(name) for name in AXES)
    grp = gx * 4 + gz * 2 + gc
    dev = dz * 4 + dy
    me = grp * 16 + dev

    def dev_peer(rel):
        other = lax.rem(dev + rel, 16)
        return (gx, gz, gc, other // 4, lax.rem(other, 4))

    def grp_peer(rel):
        other = lax.rem(grp + rel, 16)
        return (other // 4, lax.rem(other // 2, 2), lax.rem(other, 2), dz, dy)

    def y_peer(rel):
        return (gx, gz, gc, dz, lax.rem(dy + rel, 4))

    def z_peer(rel):
        return (gx, gz, gc, lax.rem(dz + rel, 4), dy)

    def ring_peer(rel):
        other = lax.rem(me + rel, 256)
        g, d = other // 16, lax.rem(other, 16)
        return (g // 4, lax.rem(g // 2, 2), lax.rem(g, 2), d // 4, lax.rem(d, 4))

    def remote(src, dst, send, recv, peer):
        return pltpu.make_async_remote_copy(
            src_ref=src,
            dst_ref=dst,
            send_sem=send,
            recv_sem=recv,
            device_id=peer,
            device_id_type=pl.DeviceIdType.MESH,
        )

    def load_a(g):
        cut = pl.ds(g * 4, 4)
        return pltpu.make_async_copy(a_hbm.at[cut], a_buf.at[cut], sem_a.at[g])

    def load_p(g):
        cut = pl.ds(g * 8, 8)
        return pltpu.make_async_copy(p_hbm.at[cut], p_buf.at[cut], sem_p.at[g])

    load_p(0).start()
    load_a(0).start()
    load_a(1).start()
    load_p(7).start()
    for g in range(1, 7):
        load_p(g).start()
        load_a(g + 1).start()

    nxt, prv = ring_peer(1), ring_peer(255)
    barrier = pltpu.get_barrier_semaphore()
    peers = [nxt, prv] + [dev_peer(k) for k in range(1, 16)] + [grp_peer(k) for k in range(1, 16)]
    with jax.named_scope("signals"):
        for peer in peers:
            pl.semaphore_signal(barrier, inc=1, device_id=peer, device_id_type=pl.DeviceIdType.MESH)

    zero_f = jnp.zeros((T, T), F32)
    zero_b = jnp.zeros((T, T), BF16)
    prod[PZ] = zero_f
    p_buf[64] = zero_f
    pt[64] = zero_b
    pt[129] = zero_b
    for side, block in ((0, 0), (1, NB - 1)):
        for slot in range(2):
            id_send[side, :, slot * T : (slot + 1) * T] = jnp.full((8, T), ids[slot, block], jnp.int32)

    def pick(block, j, first, none):
        return jnp.where(ids[0, block] == j, first, jnp.where(ids[1, block] == j, first + 1, none))

    def push_p(p0, p1, unit):
        h0, l0 = split(p0)
        h1, l1 = split(p1)
        high, low = jnp.concatenate([h0, h1], axis=1), jnp.concatenate([l0, l1], axis=1)
        pltpu.matmul_push_rhs(jnp.concatenate([high, low], axis=0), 0, unit)
        return (h0, h1), (l0, l1)

    def r_at(pair, parity):
        return (r_even, r_odd)[parity].at[pair // 2]

    def put_r(pair, parity, half, j, terms, block, extra=None):
        into = r_at(pair, parity)
        own = pick(block, j, block * 2, 64)
        total = jnp.zeros((8, T), F32)
        for k in range(4):
            rows = pl.ds(k * 32, 32)
            value = prod[terms[0], rows] + prod[terms[1], rows]
            if len(terms) == 3:
                value = value + prod[terms[2], rows]
            if extra is not None:
                value = value + extra[k * 32 : (k + 1) * 32]
            place = pl.ds(half * T + k * 32, 32)
            into[0, j, place] = value
            into[1, j, place] = rest(value)
            total = total + jnp.sum((value * p_buf[own, rows]).reshape(4, 8, T), axis=0)
        return total

    def assemble(pair, parity):
        total = jnp.zeros((8, T), F32)
        for half in range(2):
            block = pair * 2 - 1 + half
            for j in range(CT):
                terms = [pick(block - 1 + m, j, (block - 1 + m) * 6 + m * 2, PZ) for m in range(3)]
                total = total + put_r(pair, parity, half, j, terms, block)
        return total

    def body(acc, odd):

        def products(t, into):
            for unit in range(2):
                n = t * 2 + unit
                high, low = push_p(p_buf[n * 2], p_buf[n * 2 + 1], unit)
                for slot in range(2):
                    pt[n * 2 + slot] = high[slot].T
                    pt[65 + n * 2 + slot] = low[slot].T
                for m in range(3):
                    tile = a_buf[jnp.clip(n + 1 - m, 0, NB - 1), m]
                    pltpu.matmul_acc_lhs(into[unit][m], twice(tile), load_staged_rhs=0 if m == 0 else None)
                    pltpu.matmul_acc_lhs(into[unit][m], twice(rest(tile)))

        def drain(t, into):
            for unit in range(2):
                n = t * 2 + unit
                for m in range(3):
                    res = pltpu.matmul_pop(into[unit][m])
                    prod[(n * 3 + m) * 2] = res[:, :T]
                    prod[(n * 3 + m) * 2 + 1] = res[:, T:]

        def one_group(g):
            products(g * 2, acc)
            products(g * 2 + 1, odd)
            drain(g * 2, acc)
            drain(g * 2 + 1, odd)

        def two_groups(k, carry):
            for u in (1, 2):
                load_p(k * 2 + u).wait()
                load_a(k * 2 + u + 1).wait()
            t = k * 4 + 2
            products(t, acc)
            products(t + 1, odd)
            drain(t, acc)
            products(t + 2, acc)
            drain(t + 1, odd)
            products(t + 3, odd)
            drain(t + 2, acc)
            drain(t + 3, odd)
            return carry

        with jax.named_scope("load"):
            load_p(0).wait()
            load_a(0).wait()
            load_a(1).wait()
        with jax.named_scope("right_start"):
            one_group(0)
        with jax.named_scope("right_loop"):
            lax.fori_loop(0, 2, two_groups, 0)
        load_p(7).wait()
        with jax.named_scope("barrier"):
            pl.semaphore_wait(barrier, 32)
        halo_copies = [
            remote(p_buf.at[pl.ds(62, 2)], halo.at[0], sem_hs.at[0], sem_hr.at[0], nxt),
            remote(p_buf.at[pl.ds(0, 2)], halo.at[1], sem_hs.at[1], sem_hr.at[1], prv),
            remote(id_send.at[1], halo_id.at[0], sem_hs.at[2], sem_hr.at[2], nxt),
            remote(id_send.at[0], halo_id.at[1], sem_hs.at[3], sem_hr.at[3], prv),
        ]
        for copy in halo_copies:
            copy.start()
        with jax.named_scope("right_loop"):
            lax.fori_loop(2, 3, two_groups, 0)
        with jax.named_scope("right_end"):
            one_group(7)

        ends = ((0, 0), (1, 15))

        def lhs(b0, b1, i, low):
            base = 65 if low else 0
            none = 129 if low else 64
            return jnp.concatenate(
                [pt[pick(b0, i, base + b0 * 2, none)], pt[pick(b1, i, base + b1 * 2, none)]], axis=1
            )

        def pair_step(part, pair, parity, b0, b1):
            read = r_at(pair, parity)
            tiles = [lax.rem(dz + OFFSETS[part * 2 + t], 4) for t in range(2)]
            high, low = ([lhs(b0, b1, i, under) for i in tiles] for under in (False, True))
            into = (odd, acc)[part]

            def push(level):
                for unit in range(2):
                    right = jnp.concatenate([read[level, unit * 2], read[level, unit * 2 + 1]], axis=1)
                    pltpu.matmul_push_rhs(right, level, unit)

            push(0)
            for left, t, staged in ((low, 0, 0), (high, 0, None), (low, 1, None), (high, 1, None)):
                for unit in range(2):
                    pltpu.matmul_acc_lhs(into[unit][t], left[t], load_staged_rhs=staged)
            push(1)
            for left, t, staged in ((high, 1, 1), (high, 0, None)):
                for unit in range(2):
                    pltpu.matmul_acc_lhs(into[unit][t], left[t], load_staged_rhs=staged)

        def finish(part):
            for t in range(2):
                for unit in range(2):
                    res = pltpu.matmul_pop((odd, acc)[part][unit][t])
                    for y in range(4):
                        c_send[part * 2 + t, y, :, unit * 2 * T : (unit + 1) * 2 * T] = res[y * 32 : (y + 1) * 32]

        def four_first(k, total):
            for u in range(4):
                pair = k * 4 + 1 + u
                pair_step(0, pair, (1 + u) % 2, pair * 2 - 1, pair * 2)
                total = total + assemble(pair + 1, u % 2)
            return total

        def four_second(k, carry):
            for u in range(4):
                pair = lax.rem(k * 4 + 1 + u, 16)
                pair_step(1, pair, (1 + u) % 2, lax.rem(pair * 2 + 31, 32), pair * 2)
            return carry

        with jax.named_scope("assemble"):
            total = assemble(1, 1)
        with jax.named_scope("left_loop_0"):
            total = lax.fori_loop(0, 3, four_first, total)
        with jax.named_scope("left_end_0"):
            pair_step(0, 13, 1, 25, 26)
            total = total + assemble(14, 0)
            pair_step(0, 14, 0, 27, 28)
            total = total + assemble(15, 1)
            pair_step(0, 15, 1, 29, 30)

        with jax.named_scope("halo_wait"):
            for copy in halo_copies:
                copy.wait_recv()
        for side in range(2):
            push_p(halo[side, 0], halo[side, 1], side)
            tile = a_buf[0, 0] if side == 0 else a_buf[NB - 1, 2]
            pltpu.matmul_acc_lhs(acc[side][0], twice(tile), load_staged_rhs=0)
            pltpu.matmul_acc_lhs(acc[side][0], twice(rest(tile)))
        edge = [pltpu.matmul_pop(acc[side][0]) for side in range(2)]
        for side in range(2):
            prod[193 + side * 2] = edge[side][:, :T]
            prod[194 + side * 2] = edge[side][:, T:]
        inner = [dev > 0, dev < 15]
        for half, side in ((0, 1), (1, 0)):
            for j in range(CT):
                block = 0 if half == 1 else NB - 1
                terms = [pick(block, j, block * 6 + 2, PZ)]
                terms += [pick(30, j, 180, PZ)] if side == 1 else [pick(1, j, 10, PZ)]
                extra = zero_f
                for slot in range(2):
                    match = halo_id[side, 0:1, slot * T : (slot + 1) * T] == j
                    extra = extra + jnp.where(match, prod[193 + side * 2 + slot], 0.0)
                total = total + put_r(0, 0, half, j, terms, block, jnp.where(inner[side], extra, 0.0))

        def edge_y(side, rel):
            other = lax.rem(dy + rel, 4)
            return remote(
                e_send.at[side, other], e_y.at[side], sem_es.at[side, rel - 1], sem_er.at[side, 0], y_peer(rel)
            )

        def edge_z(side, rel):
            other = lax.rem(dz + rel, 4)
            return remote(
                e_pass.at[side, other], e_recv.at[side], sem_es.at[side, rel + 2], sem_er.at[side, 1], z_peer(rel)
            )

        def start_edges():
            for side, at in ends:

                @pl.when(dev == at)
                def _(side=side, at=at):
                    block = 0 if side == 0 else NB - 1
                    y0, y1 = prod[193 + side * 2], prod[194 + side * 2]
                    wide = jnp.concatenate([y0, y1], axis=1)
                    for part in (wide, rest(wide)):
                        for unit in range(2):
                            pltpu.matmul_push_rhs(jnp.concatenate([part, part], axis=0), 0, unit)
                            left = jnp.concatenate([pt[block * 2 + unit], pt[65 + block * 2 + unit]], axis=1)
                            pltpu.matmul_acc_lhs(acc[unit][0], left, load_staged_rhs=0)
                    for unit in range(2):
                        res = pltpu.matmul_pop(acc[unit][0])
                        for y in range(4):
                            e_send[side, y, unit * 32 : (unit + 1) * 32] = res[y * 32 : (y + 1) * 32]
                    upper = lax.broadcasted_iota(jnp.int32, (8, 2 * T), 0) < 4
                    code = jnp.where(upper, halo_id[side], id_send[side]).astype(F32)
                    for y in range(4):
                        e_send[side, y, 64:72] = code
                    for rel in range(1, 4):
                        edge_y(side, rel).start()
                    e_y[side] = e_send[side, at % 4]

        def pass_edges():
            for side, at in ends:

                @pl.when(dz == at // 4)
                def _(side=side, at=at):
                    @pl.when(dy != at % 4)
                    def _():
                        edge_y(side, 1).wait_recv()

                    for z in range(4):
                        for part in range(2):
                            half = slice(part * T, (part + 1) * T)
                            value = jnp.zeros((32, T), F32)
                            for slot in range(2):
                                match = e_y[side, 68:69, slot * T : (slot + 1) * T] == float(z)
                                value = value + jnp.where(match, e_y[side, slot * 32 : (slot + 1) * 32, half], 0.0)
                            e_pass[side, z, 0:32, half] = value
                        e_pass[side, z, 32:40] = e_y[side, 64:72]
                    for rel in range(1, 4):
                        edge_z(side, rel).start()
                    e_recv[side] = e_pass[side, at // 4]

        def t_copies(phase):
            row = pl.ds(0, 1)
            peer = (dev_peer, grp_peer)[phase]
            return [
                remote(
                    t_send.at[phase, row],
                    t_recv.at[phase, rel, row],
                    sem_ts.at[phase, rel],
                    sem_tr.at[phase, rel],
                    peer(rel),
                )
                for rel in range(1, 16)
            ]

        def t_begin(phase, total):
            t_send[phase, 0:1] = total
            start(t_copies(phase))

        def t_sum(phase, total):
            for rel, copy in enumerate(t_copies(phase)):
                copy.wait_recv()
                total = total + t_recv[phase, rel + 1, 0:1]
            return total

        def start(copies):
            for copy in copies:
                copy.start()

        total = jnp.sum(total, axis=0, keepdims=True)
        t_begin(0, total)
        pair_step(0, 0, 0, NB - 1, 0)
        finish(0)

        def y_all(c):
            return [
                remote(
                    c_send.at[c, lax.rem(dy + rel, 4)],
                    y_recv.at[c, rel - 1],
                    sem_ys.at[c, rel - 1],
                    sem_yr.at[c, rel - 1],
                    y_peer(rel),
                )
                for rel in range(1, 4)
            ]

        def z_one(c):
            return remote(z_send.at[c], z_recv.at[c], sem_zs.at[c], sem_zr.at[c], z_peer(OFFSETS[c]))

        def y_sum(c):
            value = c_send[c, dy]
            for k, copy in enumerate(y_all(c)):
                copy.wait_recv()
                value = value + y_recv[c, k]
            return value

        def begin_z(c):
            z_send[c] = y_sum(c)
            z_one(c).start()

        start(y_all(0))
        with jax.named_scope("edges"):
            start_edges()
        start(y_all(1))
        with jax.named_scope("left_loop"):
            lax.fori_loop(0, 4, four_second, 0)
            finish(1)
        start(y_all(2))
        start(y_all(3))
        with jax.named_scope("z_0"):
            begin_z(0)
        with jax.named_scope("trace_dev"):
            total = t_sum(0, total)
            t_begin(1, total)
        with jax.named_scope("edge_pass"):
            pass_edges()
        with jax.named_scope("z_1"):
            begin_z(1)
        with jax.named_scope("z_2"):
            begin_z(2)
        with jax.named_scope("y_3"):
            mine = y_sum(3)
        with jax.named_scope("trace_grp"):
            total = t_sum(1, total)
        mean = jnp.sum(total, axis=(0, 1), keepdims=True) * (1.0 / 8192.0)
        scale = jnp.broadcast_to(mean, (32, 2 * T))

        for side, at in ends:
            base = 0 if side == 0 else 1024

            with jax.named_scope("edge_wait"):

                @pl.when(dz != at // 4)
                def _(side=side):
                    edge_z(side, 1).wait_recv()

            for j in range(CT):
                value = jnp.zeros((32, T), F32)
                for slot in range(2):
                    match = e_recv[side, 32:33, slot * T : (slot + 1) * T] == float(j)
                    value = value + jnp.where(match, e_recv[side, 0:32, slot * T : (slot + 1) * T], 0.0)
                out[:, base + j * T : base + (j + 1) * T] = value / scale[:, :T]

        with jax.named_scope("z_wait"):
            for c in range(3):
                z_one(c).wait_recv()
                mine = mine + z_recv[c]
        out[:, 512:1024] = mine / jnp.broadcast_to(mean, (32, 4 * T))

        done = jax.named_scope("sends_done")
        done.__enter__()
        for copy in halo_copies + t_copies(0) + t_copies(1):
            copy.wait_send()
        for c in range(4):
            for copy in y_all(c):
                copy.wait_send()
        for c in range(3):
            z_one(c).wait_send()
        for side, at in ends:

            @pl.when(dev == at)
            def _(side=side):
                for rel in range(1, 4):
                    edge_y(side, rel).wait_send()

            @pl.when(dz == at // 4)
            def _(side=side):
                for rel in range(1, 4):
                    edge_z(side, rel).wait_send()

        done.__exit__(None, None, None)

    small, other = (
        tuple(tuple(pltpu.ACC(unit)((T, 2 * T), F32) for _ in range(3)) for unit in range(2)) for _ in range(2)
    )
    pl.run_scoped(body, small, other)


def local(a_tiles, prolong, coarse_ids):
    vmem, dma = pltpu.VMEM, pltpu.SemaphoreType.DMA
    return pl.pallas_call(
        kernel,
        out_shape=jax.ShapeDtypeStruct((32, 1536), F32),
        in_specs=[
            pl.BlockSpec(memory_space=pltpu.SMEM),
            pl.BlockSpec(memory_space=pltpu.HBM),
            pl.BlockSpec(memory_space=pltpu.HBM),
        ],
        out_specs=pl.BlockSpec(memory_space=pltpu.VMEM),
        scratch_shapes=[
            vmem((NB, 3, T, T), F32),
            vmem((65, T, T), F32),
            vmem((130, T, T), BF16),
            vmem((197, T, T), F32),
            vmem((8, 2, 4, 2 * T, T), F32),
            vmem((8, 2, 4, 2 * T, T), F32),
            vmem((2, 2, T, T), F32),
            vmem((2, 8, 2 * T), jnp.int32),
            vmem((2, 8, 2 * T), jnp.int32),
            vmem((4, 4, 32, 4 * T), F32),
            vmem((4, 3, 32, 4 * T), F32),
            vmem((3, 32, 4 * T), F32),
            vmem((3, 32, 4 * T), F32),
            vmem((2, 4, 72, 2 * T), F32),
            vmem((2, 72, 2 * T), F32),
            vmem((2, 4, 40, 2 * T), F32),
            vmem((2, 40, 2 * T), F32),
            vmem((2, 8, T), F32),
            vmem((2, 16, 8, T), F32),
            dma((8,)),
            dma((8,)),
            dma((4,)),
            dma((4,)),
            dma((4, 3)),
            dma((4, 3)),
            dma((3,)),
            dma((3,)),
            dma((2, 6)),
            dma((2, 2)),
            dma((2, 16)),
            dma((2, 16)),
        ],
        compiler_params=pltpu.CompilerParams(
            collective_id=0, has_side_effects=True, vmem_limit_bytes=VMEM_MIB * 1024 * 1024
        ),
    )(coarse_ids.T, a_tiles, prolong.reshape(2 * NB, T, T))


def solution(mesh):
    torus = Mesh(mesh.devices.reshape(4, 2, 2, 4, 4), GRP_DEV)

    def run(a_tiles, prolong, coarse_ids):
        return jax.shard_map(
            local,
            mesh=torus,
            in_specs=(P(GRP_DEV, None, None, None), P(GRP_DEV, None, None, None), P(GRP_DEV, None)),
            out_specs=P(GRP_DEV, None),
            check_vma=False,
        )(a_tiles, prolong, coarse_ids)

    return run
```
